128 devices in a mesh: replica: 1, dp: 128 (over z, y, x, core).
Axes of the slice: x: 4, y: 4, z: 4, core: 2. Of those that a mesh axis runs over, the one named last changes fastest.
Arguments:
- x_rows: bfloat16 [256, 2048], P(('replica', 'dp'))
- lengths: int32 [256], P(('replica', 'dp'))
- cache0: bfloat16 [256, 1024, 576], P(('replica', 'dp'))
- cache1: bfloat16 [256, 1024, 576], P(('replica', 'dp'))
- attn_gain: float32 [2, 2048], replicated
- w_dkv: bfloat16 [2, 2048, 576], replicated
- kv_gain: float32 [2, 512], replicated
- wq_a: bfloat16 [2, 2048, 768], replicated
- q_gain: float32 [2, 768], replicated
- wq_b: bfloat16 [2, 768, 5120], replicated
- w_uk: bfloat16 [2, 20, 192, 512], replicated
- w_uv: bfloat16 [2, 20, 512, 256], replicated
- w_o: bfloat16 [2, 5120, 2048], replicated
- ffn_gain: float32 [2, 2048], replicated
- w_gate: bfloat16 [2, 2048, 10240], replicated
- w_up: bfloat16 [2, 2048, 10240], replicated
- w_down: bfloat16 [2, 10240, 2048], replicated
Outputs:
- output 1: bfloat16 [256, 2048], P('replica')
- output 2: bfloat16 [256, 1024, 576], P(('replica', 'dp'))
- output 3: bfloat16 [256, 1024, 576], P(('replica', 'dp'))
All inputs are finite; a program needn't handle non-finite values.
Results may differ from the reference program's by a relative error of at most 0.02.
Values are sent between devices in bfloat16 or wider.
A program may use at most 1.5 GiB of HBM per device.

```python
import functools
import jax
import jax.numpy as jnp
from jax import lax

GROUP_SIZE = 128
ROWS_DEV = 2
SEQ_LEN = 1024
MODEL_DIM = 2048
FFN_DIM = 10240
NUM_HEADS = 20
Q_RANK = 768
KV_RANK = 512
NOPE_DIM = 192
ROPE_DIM = 64
VALUE_DIM = 256
LAYER_COUNT = 2

BATCH_ROWS = GROUP_SIZE * ROWS_DEV
CACHE_DIM = KV_RANK + ROPE_DIM
QK_DIM = NOPE_DIM + ROPE_DIM


def rms_norm(values, gain_vec):
    return values * lax.rsqrt(jnp.mean(values * values, axis=-1, keepdims=True) + 1e-6) * gain_vec


def apply_rope(values, positions):
    half_dim = values.shape[-1] // 2
    inv_freq = 10000.0 ** (-jnp.arange(half_dim, dtype=jnp.float32) / half_dim)
    angles = positions.astype(jnp.float32)[..., None] * inv_freq
    cos_a = jnp.cos(angles)
    sin_a = jnp.sin(angles)
    first_half = values[..., :half_dim]
    second_half = values[..., half_dim:]
    return jnp.concatenate([first_half * cos_a - second_half * sin_a, second_half * cos_a + first_half * sin_a], axis=-1)


def attention_block(block_in, layer_w):
    residual, lengths, layer_cache = block_in
    attn_gain, w_dkv, kv_gain, wq_a, q_gain, wq_b, w_uk, w_uv, w_o = layer_w
    num_rows = residual.shape[0]
    hidden = rms_norm(residual.astype(jnp.float32), attn_gain).astype(jnp.bfloat16)
    kv_proj = jnp.dot(hidden, w_dkv, preferred_element_type=jnp.float32)
    latent = rms_norm(kv_proj[:, :KV_RANK], kv_gain).astype(jnp.bfloat16)
    key_rope = apply_rope(kv_proj[:, KV_RANK:], lengths).astype(jnp.bfloat16)
    new_entry = jnp.concatenate([latent, key_rope], axis=-1)
    slot_ids = jnp.arange(SEQ_LEN, dtype=jnp.int32)[None, :]
    at_slot = slot_ids == lengths[:, None]
    cache_new = jnp.where(at_slot[:, :, None], new_entry[:, None, :], layer_cache)
    q_low = rms_norm(jnp.dot(hidden, wq_a, preferred_element_type=jnp.float32), q_gain).astype(jnp.bfloat16)
    queries = jnp.dot(q_low, wq_b, preferred_element_type=jnp.float32).astype(jnp.bfloat16).reshape(num_rows, NUM_HEADS, QK_DIM)
    q_rope = apply_rope(queries[:, :, NOPE_DIM:].astype(jnp.float32), lengths[:, None]).astype(jnp.bfloat16)
    q_latent = jnp.einsum('bhn,hnk->bhk', queries[:, :, :NOPE_DIM].astype(jnp.float32), w_uk.astype(jnp.float32)).astype(jnp.bfloat16)
    q_full = jnp.concatenate([q_latent, q_rope], axis=-1)
    scores = jnp.einsum('bhc,btc->bht', q_full.astype(jnp.float32), cache_new.astype(jnp.float32)) * (QK_DIM ** -0.5)
    visible = slot_ids <= lengths[:, None]
    scores = jnp.where(visible[:, None, :], scores, -1e30)
    attn_probs = jax.nn.softmax(scores, axis=-1).astype(jnp.bfloat16)
    out_latent = jnp.einsum('bht,btk->bhk', attn_probs.astype(jnp.float32), cache_new[:, :, :KV_RANK].astype(jnp.float32)).astype(jnp.bfloat16)
    heads_out = jnp.einsum('bhk,hkv->bhv', out_latent.astype(jnp.float32), w_uv.astype(jnp.float32)).astype(jnp.bfloat16).reshape(num_rows, NUM_HEADS * VALUE_DIM)
    attn_out = jnp.dot(heads_out, w_o, preferred_element_type=jnp.float32)
    return (residual.astype(jnp.float32) + attn_out).astype(jnp.bfloat16), cache_new


def mlp_block(residual, ffn_gain, w_gate, w_up, w_down):
    normed = rms_norm(residual.astype(jnp.float32), ffn_gain).astype(jnp.bfloat16)
    gate_proj = jnp.dot(normed, w_gate, preferred_element_type=jnp.float32)
    up_proj = jnp.dot(normed, w_up, preferred_element_type=jnp.float32)
    activated = (jax.nn.silu(gate_proj) * up_proj).astype(jnp.bfloat16)
    mlp_out = jnp.dot(activated, w_down, preferred_element_type=jnp.float32)
    return (residual.astype(jnp.float32) + mlp_out).astype(jnp.bfloat16)


def draw_normal(rng_key, arr_shape, scale_by):
    return (scale_by * jax.random.normal(rng_key, arr_shape, jnp.float32)).astype(jnp.bfloat16)


def draw_gain(rng_key, arr_shape):
    return 1.0 + 0.5 * jax.random.normal(rng_key, arr_shape, jnp.float32)


def draw_lengths(len_key):
    key_short, key_long, key_pick = jax.random.split(len_key, 3)
    short_len = jax.random.randint(key_short, (BATCH_ROWS,), 0, 8)
    long_len = jax.random.randint(key_long, (BATCH_ROWS,), 0, SEQ_LEN)
    pick_short = jax.random.randint(key_pick, (BATCH_ROWS,), 0, 2) == 0
    drawn = jnp.where(pick_short, short_len, long_len)
    return jnp.where(jnp.arange(BATCH_ROWS) == 0, SEQ_LEN - 1, drawn).astype(jnp.int32)


def draw_cache(cache_key, lengths):
    key_valid, key_junk = jax.random.split(cache_key)
    arr_shape = (BATCH_ROWS, SEQ_LEN, CACHE_DIM)
    valid_vals = jax.random.normal(key_valid, arr_shape, jnp.float32)
    junk_vals = 20.0 * jax.random.normal(key_junk, arr_shape, jnp.float32)
    is_live = jnp.arange(SEQ_LEN)[None, :, None] < lengths[:, None, None]
    return jnp.where(is_live, valid_vals, junk_vals).astype(jnp.bfloat16)


def setup_inputs(seed: int = 0, part: int = 0) -> dict:
    base_key = jax.random.key(seed)
    part_keys = jax.random.split(jax.random.fold_in(base_key, part), 4)
    shared_keys = jax.random.split(base_key, 13)
    lengths = draw_lengths(part_keys[1])
    return {
        'x_rows': draw_normal(part_keys[0], (BATCH_ROWS, MODEL_DIM), 1.0),
        'lengths': lengths,
        'cache0': draw_cache(part_keys[2], lengths),
        'cache1': draw_cache(part_keys[3], lengths),
        'attn_gain': draw_gain(shared_keys[0], (LAYER_COUNT, MODEL_DIM)),
        'w_dkv': draw_normal(shared_keys[1], (LAYER_COUNT, MODEL_DIM, CACHE_DIM), MODEL_DIM ** -0.5),
        'kv_gain': draw_gain(shared_keys[2], (LAYER_COUNT, KV_RANK)),
        'wq_a': draw_normal(shared_keys[3], (LAYER_COUNT, MODEL_DIM, Q_RANK), MODEL_DIM ** -0.5),
        'q_gain': draw_gain(shared_keys[4], (LAYER_COUNT, Q_RANK)),
        'wq_b': draw_normal(shared_keys[5], (LAYER_COUNT, Q_RANK, NUM_HEADS * QK_DIM), Q_RANK ** -0.5),
        'w_uk': draw_normal(shared_keys[6], (LAYER_COUNT, NUM_HEADS, NOPE_DIM, KV_RANK), 1.5 * NOPE_DIM ** -0.5),
        'w_uv': draw_normal(shared_keys[7], (LAYER_COUNT, NUM_HEADS, KV_RANK, VALUE_DIM), KV_RANK ** -0.5),
        'w_o': draw_normal(shared_keys[8], (LAYER_COUNT, NUM_HEADS * VALUE_DIM, MODEL_DIM), 1.5 * (NUM_HEADS * VALUE_DIM) ** -0.5),
        'ffn_gain': draw_gain(shared_keys[9], (LAYER_COUNT, MODEL_DIM)),
        'w_gate': draw_normal(shared_keys[10], (LAYER_COUNT, MODEL_DIM, FFN_DIM), MODEL_DIM ** -0.5),
        'w_up': draw_normal(shared_keys[11], (LAYER_COUNT, MODEL_DIM, FFN_DIM), MODEL_DIM ** -0.5),
        'w_down': draw_normal(shared_keys[12], (LAYER_COUNT, FFN_DIM, MODEL_DIM), 1.5 * FFN_DIM ** -0.5),
    }


def reference(x_rows, lengths, cache0, cache1, attn_gain, w_dkv, kv_gain, wq_a, q_gain, wq_b, w_uk, w_uv, w_o, ffn_gain, w_gate, w_up, w_down):
    residual = x_rows
    caches_in = (cache0, cache1)
    new_caches = []
    for layer_idx in range(LAYER_COUNT):
        layer_w = (attn_gain[layer_idx], w_dkv[layer_idx], kv_gain[layer_idx], wq_a[layer_idx], q_gain[layer_idx], wq_b[layer_idx], w_uk[layer_idx], w_uv[layer_idx], w_o[layer_idx])
        blocks = (residual.reshape(GROUP_SIZE, ROWS_DEV, MODEL_DIM), lengths.reshape(GROUP_SIZE, ROWS_DEV), caches_in[layer_idx].reshape(GROUP_SIZE, ROWS_DEV, SEQ_LEN, CACHE_DIM))
        block_out, block_cache = lax.map(functools.partial(attention_block, layer_w=layer_w), blocks)
        new_caches.append(block_cache.reshape(BATCH_ROWS, SEQ_LEN, CACHE_DIM))
        residual = mlp_block(block_out.reshape(BATCH_ROWS, MODEL_DIM), ffn_gain[layer_idx], w_gate[layer_idx], w_up[layer_idx], w_down[layer_idx])
    return residual, new_caches[0], new_caches[1]
```

```python
import functools

import jax
import jax.numpy as jnp
import numpy as np
from jax import lax
from jax.experimental import pallas as pl
from jax.experimental.pallas import tpu as pltpu
from jax.sharding import PartitionSpec as P

BF = jnp.bfloat16
F32 = jnp.float32
MESH = pl.DeviceIdType.MESH
NT = (((1,), (1,)), ((), ()))

SEQ = 1024
DIM = 2048
FFN = 10240
HEADS = 20
KVR = 512
NOPE = 192
ROPE = 64
QKD = NOPE + ROPE
CACHE = KVR + ROPE
QR = 768
VD = 256
ROWS = 2
PAD = 16
HP = 32
GROUP = 16
FS = FFN // GROUP
QB = 4
KC = 512
WOC = HEADS * VD // KC
AHEAD = 9


def rms(v, gain):
    return v * lax.rsqrt(jnp.mean(v * v, axis=-1, keepdims=True) + 1e-6) * gain


def rope_lanes(t, cos_t, sin_t):
    lane = lax.broadcasted_iota(jnp.int32, t.shape, 1)
    swapped = jnp.where(lane < ROPE // 2, pltpu.roll(t, 128 - ROPE // 2, 1), pltpu.roll(t, ROPE // 2, 1))
    return t * cos_t + swapped * sin_t


def attn_kernel(layer, len_ref, x_ref, freq_ref, ag_ref, kvg_ref, qg_ref, cache_ref, wdkv_ref, wqa_ref, wqb_ref, wuk_ref, wuv_ref, wo_ref,
                xo_ref, co_ref,
                wdkv, wqa, wqb, wuk, wuv, wo, cbuf, xs, ks, qf, qlat, qrs, of, ob, acc, sems, out_sem):
    half = HEADS // 2
    qc = HEADS * QKD // QB
    chunks = [(wdkv_ref.at[layer], wdkv), (wqa_ref.at[layer], wqa)]
    chunks += [(wqb_ref.at[layer, :, pl.ds(i * qc, qc)], wqb.at[:, pl.ds(i * qc, qc)]) for i in range(QB)]
    chunks += [(wuk_ref.at[layer, pl.ds(i * half, half)], wuk.at[pl.ds(i * half, half)]) for i in range(2)]
    chunks += [(cache_ref, cbuf)]
    chunks += [(wuv_ref.at[layer, pl.ds(i * half, half)], wuv.at[pl.ds(i * half, half)]) for i in range(2)]
    first_wo = len(chunks)
    chunks += [(wo_ref.at[layer, pl.ds(i * KC, KC)], wo.at[pl.ds(i * KC, KC)]) for i in range(WOC)]
    copies = [pltpu.make_async_copy(s, d, sems.at[i]) for i, (s, d) in enumerate(chunks)]
    for cp in copies[:AHEAD]:
        cp.start()

    def ready(i):
        copies[i].wait()
        if i + AHEAD < len(copies):
            copies[i + AHEAD].start()

    xs[...] = jnp.zeros_like(xs)
    xs[0:ROWS, :] = x_ref[...].astype(F32)
    ks[...] = jnp.zeros_like(ks)
    of[...] = jnp.zeros_like(of)
    for b in range(ROWS):
        qlat[b, 16:HP, :] = jnp.zeros((HP - 16, KVR), F32)
        qrs[b, 16:HP, :] = jnp.zeros((HP - 16, 128), F32)
    h = rms(xs[...], ag_ref[layer:layer + 1, :]).astype(BF)
    lane16 = lax.broadcasted_iota(jnp.int32, (PAD, 128), 1)
    row16 = lax.broadcasted_iota(jnp.int32, (PAD, 128), 0)
    angle = jnp.where(row16 == 0, len_ref[0], len_ref[1]).astype(F32) * freq_ref[...]
    cos_t = jnp.where(lane16 < ROPE, jnp.cos(angle), 0.0)
    sin_t = jnp.sin(angle)
    sin_t = jnp.where(lane16 < ROPE, jnp.where(lane16 < ROPE // 2, -sin_t, sin_t), 0.0)
    ready(0)
    k = lax.dot_general(h, wdkv[...], NT, preferred_element_type=F32)
    ready(1)
    qa = jnp.dot(h, wqa[...], preferred_element_type=F32)
    qa = rms(qa, qg_ref[layer:layer + 1, :]).astype(BF)
    ks[:, 0:CACHE] = k
    ks[:, 0:KVR] = rms(k[:, 0:KVR], kvg_ref[layer:layer + 1, :]).astype(BF).astype(F32)
    ks[:, KVR:KVR + 128] = rope_lanes(ks[:, KVR:KVR + 128], cos_t, sin_t).astype(BF).astype(F32)

    heads_q = HEADS // QB
    qparts = []
    for i in range(QB):
        ready(2 + i)
        qi = jnp.dot(qa, wqb[:, i * qc:(i + 1) * qc], preferred_element_type=F32).astype(BF)
        qf[:, i * qc:(i + 1) * qc] = qi.astype(F32)
        qparts.append(qi)
    for j in range(HEADS):
        if j % half == 0:
            ready(2 + QB + j // half)
        jj = j % heads_q
        qn = qparts[j // heads_q][:, jj * QKD:jj * QKD + NOPE]
        ql = jnp.dot(qn, wuk[j], preferred_element_type=F32)
        for b in range(ROWS):
            qlat[b, j:j + 1, :] = ql[b:b + 1, :]
            qrs[b, j:j + 1, :] = qf[b:b + 1, j * QKD + 128:(j + 1) * QKD]

    ready(4 + QB)
    ol = []
    outs = []
    ne = ks[:, 0:CACHE].astype(BF)
    for b in range(ROWS):
        p = len_ref[b]
        base = pl.multiple_of((p // 128) * 128, 128)
        hot = jnp.where((row16 == b) & (lane16 == p - base), 1.0, 0.0).astype(BF)
        col = lax.dot_general(ne, hot, (((0,), (0,)), ((), ())), preferred_element_type=F32)
        lane = lax.broadcasted_iota(jnp.int32, (CACHE, 128), 1)
        blk = cbuf[b, :, pl.ds(base, 128)].astype(F32)
        cbuf[b, :, pl.ds(base, 128)] = jnp.where(lane == p - base, col, blk).astype(BF)
    for b in range(ROWS):
        p = len_ref[b]
        qr = rope_lanes(pltpu.roll(qrs[b], 64, 1), cos_t[b:b + 1, :], sin_t[b:b + 1, :]).astype(BF)
        s = jnp.dot(qlat[b].astype(BF), cbuf[b, 0:KVR, :], preferred_element_type=F32)
        s += jnp.dot(qr[:, 0:ROPE], cbuf[b, KVR:CACHE, :], preferred_element_type=F32)
        s = s * (QKD ** -0.5)
        slot = lax.broadcasted_iota(jnp.int32, (HP, SEQ), 1)
        s = jnp.where(slot <= p, s, -1e30)
        e = jnp.exp(s - jnp.max(s, axis=-1, keepdims=True))
        a = (e / jnp.sum(e, axis=-1, keepdims=True)).astype(BF)
        ol.append(lax.dot_general(a, cbuf[b, 0:KVR, :], NT, preferred_element_type=F32).astype(BF))
        cp = pltpu.make_async_copy(cbuf.at[b], co_ref.at[b], out_sem.at[b])
        cp.start()
        outs.append(cp)
    olc = jnp.concatenate(ol, axis=0)
    for j in range(HEADS):
        if j % half == 0:
            ready(5 + QB + j // half)
        r = jnp.dot(olc, wuv[j], preferred_element_type=F32)
        for b in range(ROWS):
            of[b:b + 1, j * VD:(j + 1) * VD] = r[b * HP + j:b * HP + j + 1, :]
    for i in range(WOC):
        ob[i] = of[:, i * KC:(i + 1) * KC].astype(BF)
    acc[...] = jnp.zeros_like(acc)
    for i in range(first_wo, len(copies) - AHEAD):
        ready(i)
    late = max(first_wo, len(copies) - AHEAD)

    def step(i, carry):
        at = pl.ds(pl.multiple_of(i * KC, KC), KC)

        @pl.when(i >= late - first_wo)
        def _():
            pltpu.make_async_copy(wo_ref.at[layer, at], wo.at[at], sems.at[first_wo + i]).wait()

        acc[...] += jnp.dot(ob[i], wo[at, :], preferred_element_type=F32)
        return carry

    lax.fori_loop(0, WOC, step, 0)
    xo_ref[...] = (xs[0:ROWS, :] + acc[0:ROWS, :]).astype(BF)
    for cp in outs:
        cp.wait()


def attention(layer, lengths, x, freq, ag, kvg, qg, cache, wdkv, wqa, wqb, wuk, wuv, wo):
    vm = pl.BlockSpec(memory_space=pltpu.VMEM)
    anyspec = pl.BlockSpec(memory_space=pl.ANY)
    n_copies = 2 + QB + 2 + 1 + 2 + WOC
    wbytes = 2 * (DIM * CACHE + DIM * QR + QR * HEADS * QKD + HEADS * NOPE * KVR + HEADS * KVR * VD + HEADS * VD * DIM)
    return pl.pallas_call(
        functools.partial(attn_kernel, layer),
        out_shape=(jax.ShapeDtypeStruct((ROWS, DIM), BF), jax.ShapeDtypeStruct((ROWS, CACHE, SEQ), BF)),
        in_specs=[pl.BlockSpec(memory_space=pltpu.SMEM)] + [vm] * 5 + [anyspec] * 7,
        out_specs=(vm, anyspec),
        scratch_shapes=[
            pltpu.VMEM((CACHE, DIM), BF), pltpu.VMEM((DIM, QR), BF), pltpu.VMEM((QR, HEADS * QKD), BF),
            pltpu.VMEM((HEADS, NOPE, KVR), BF), pltpu.VMEM((HEADS, KVR, VD), BF), pltpu.VMEM((HEADS * VD, DIM), BF),
            pltpu.VMEM((ROWS, CACHE, SEQ), BF), pltpu.VMEM((PAD, DIM), F32), pltpu.VMEM((PAD, KVR + 128), F32),
            pltpu.VMEM((PAD, HEADS * QKD), F32), pltpu.VMEM((ROWS, HP, KVR), F32), pltpu.VMEM((ROWS, HP, 128), F32),
            pltpu.VMEM((PAD, HEADS * VD), F32), pltpu.VMEM((WOC, PAD, KC), BF), pltpu.VMEM((PAD, DIM), F32),
            pltpu.SemaphoreType.DMA((n_copies,)), pltpu.SemaphoreType.DMA((ROWS,)),
        ],
        compiler_params=pltpu.CompilerParams(vmem_limit_bytes=62 * 1024 * 1024),
        cost_estimate=pl.CostEstimate(flops=wbytes * 2, bytes_accessed=wbytes, transcendentals=0),
        name=f"attn{layer}",
    )(lengths, x, freq, ag, kvg, qg, cache, wdkv, wqa, wqb, wuk, wuv, wo)


def dev(i):
    return (lax.axis_index("replica"), i)


def remote(src, dst, send_sem, recv_sem, peer):
    return pltpu.make_async_remote_copy(src_ref=src, dst_ref=dst, send_sem=send_sem, recv_sem=recv_sem, device_id=dev(peer), device_id_type=MESH)


def mlp_kernel(layer, final, x_ref, gain_ref, wg_ref, wu_ref, wd_ref, out_ref, xg, xf, wg, wu, wd, pf, ps, pr, fb, wsem, s1, r1, s2, r2, fs, fr, os_):
    idx = lax.axis_index("dp")
    me = lax.rem(idx, GROUP)
    first = idx - me
    core = lax.rem(idx, 2)
    cx = lax.rem(lax.div(idx, 2), 4)
    cy = lax.rem(lax.div(idx, 8), 4)
    cz = lax.div(idx, 32)
    at = pl.ds(pl.multiple_of(me * FS, FS), FS)
    loads = [pltpu.make_async_copy(wg_ref.at[layer, :, at], wg, wsem.at[0]),
             pltpu.make_async_copy(wu_ref.at[layer, :, at], wu, wsem.at[1]),
             pltpu.make_async_copy(wd_ref.at[layer, at, :], wd, wsem.at[2])]
    for cp in loads:
        cp.start()

    def rank(k):
        return lax.rem(me + k, GROUP)

    peers = [first + rank(k) for k in range(1, GROUP)]
    if final:
        other = lax.rem(lax.div(cy, 2) + 1, 2) * 2
        peers += [cz * 32 + (other + k) * 8 + cx * 2 + core for k in range(2)]
        peers += [lax.rem(cz + k, 4) * 32 + cy * 8 + cx * 2 + core for k in range(1, 4)]
    barrier = pltpu.get_barrier_semaphore()
    for p in peers:
        pl.semaphore_signal(barrier, inc=1, device_id=dev(p), device_id_type=MESH)
    pl.semaphore_wait(barrier, len(peers))

    order = sorted(range(1, GROUP), key=lambda k: -min(k, GROUP - k))
    sends = {}
    for k in order:
        sends[k] = remote(x_ref, xg.at[me], s1.at[k], r1.at[k], first + rank(k))
        sends[k].start()
    xg[me] = x_ref[...]
    for k in range(1, GROUP):
        src = rank(GROUP - k)
        remote(x_ref, xg.at[src], s1.at[k], r1.at[k], first + src).wait_recv()
    for d in range(GROUP):
        xf[ROWS * d:ROWS * (d + 1), :] = xg[d].astype(F32)
    g = rms(xf[...], gain_ref[layer:layer + 1, :]).astype(BF)
    loads[0].wait()
    gate = jnp.dot(g, wg[...], preferred_element_type=F32)
    loads[1].wait()
    up = jnp.dot(g, wu[...], preferred_element_type=F32)
    u = (gate * jax.nn.sigmoid(gate) * up).astype(BF)
    loads[2].wait()
    pf[...] = jnp.dot(u, wd[...], preferred_element_type=F32)
    for d in range(GROUP):
        ps[d] = pf[ROWS * d:ROWS * (d + 1), :].astype(BF)
    back = {}
    for k in order:
        dst = rank(k)
        back[k] = remote(ps.at[dst], pr.at[me], s2.at[k], r2.at[k], first + dst)
        back[k].start()
    pr[me] = ps[me]
    for k in range(1, GROUP):
        src = rank(GROUP - k)
        remote(ps.at[src], pr.at[src], s2.at[k], r2.at[k], first + src).wait_recv()
    total = pr[0].astype(F32)
    for d in range(1, GROUP):
        total += pr[d].astype(F32)
    fin = (x_ref[...].astype(F32) + total).astype(BF)
    if not final:
        out_ref[...] = fin
    else:
        fb[core, cz, cy, cx] = fin
        partner = idx + 1 - 2 * core
        started = []

        def stage(n, slot_of, peer_of):
            for k in range(1, 4):
                cp = remote(slot_of(0), slot_of(0), fs.at[n, k], fr.at[n, k], peer_of(k))
                cp.start()
                started.append(cp)
            return [remote(slot_of(4 - k), slot_of(4 - k), fs.at[n, k], fr.at[n, k], peer_of(4 - k)) for k in range(1, 4)]

        def xs(k):
            return fb.at[core, cz, cy, lax.rem(cx + k, 4)]

        def ys(k):
            return fb.at[core, cz, lax.rem(cy + k, 4)]

        def zs(k):
            return fb.at[core, lax.rem(cz + k, 4)]

        for cp in stage(0, xs, lambda k: cz * 32 + cy * 8 + lax.rem(cx + k, 4) * 2 + core):
            cp.wait_recv()
        for cp in stage(1, ys, lambda k: cz * 32 + lax.rem(cy + k, 4) * 8 + cx * 2 + core):
            cp.wait_recv()
        arrivals = stage(2, zs, lambda k: lax.rem(cz + k, 4) * 32 + cy * 8 + cx * 2 + core)
        outs = []

        def put(c, z, n):
            cp = pltpu.make_async_copy(fb.at[c, z], out_ref.at[z, :, :, c], os_.at[n])
            cp.start()
            outs.append(cp)

        def share(k):
            z = lax.rem(cz + k, 4)
            cp = remote(fb.at[core, z], fb.at[core, z], fs.at[3, k], fr.at[3, k], partner)
            cp.start()
            started.append(cp)
            put(core, z, k)

        share(0)
        for k in range(1, 4):
            arrivals[k - 1].wait_recv()
            share(4 - k)
        for k in (0, 3, 2, 1):
            z = lax.rem(cz + k, 4)
            remote(fb.at[1 - core, z], fb.at[1 - core, z], fs.at[3, k], fr.at[3, k], partner).wait_recv()
            put(1 - core, z, 4 + k)
        for cp in started:
            cp.wait_send()
        for cp in outs:
            cp.wait()
    for k in order:
        sends[k].wait_send()
        back[k].wait_send()


def mlp(layer, final, x, gain, wg, wu, wd):
    vm = pl.BlockSpec(memory_space=pltpu.VMEM)
    anyspec = pl.BlockSpec(memory_space=pl.ANY)
    out = jax.ShapeDtypeStruct((4, 4, 4, 2, ROWS, DIM) if final else (ROWS, DIM), BF)
    dma = pltpu.SemaphoreType.DMA
    return pl.pallas_call(
        functools.partial(mlp_kernel, layer, final),
        out_shape=out,
        in_specs=[vm, vm, anyspec, anyspec, anyspec],
        out_specs=anyspec if final else vm,
        scratch_shapes=[
            pltpu.VMEM((GROUP, ROWS, DIM), BF), pltpu.VMEM((GROUP * ROWS, DIM), F32),
            pltpu.VMEM((DIM, FS), BF), pltpu.VMEM((DIM, FS), BF), pltpu.VMEM((FS, DIM), BF),
            pltpu.VMEM((GROUP * ROWS, DIM), F32), pltpu.VMEM((GROUP, ROWS, DIM), BF), pltpu.VMEM((GROUP, ROWS, DIM), BF),
            pltpu.VMEM((2, 4, 4, 4, ROWS, DIM) if final else (1, ROWS, DIM), BF),
            dma((3,)), dma((GROUP,)), dma((GROUP,)), dma((GROUP,)), dma((GROUP,)), dma((4, 4)), dma((4, 4)), dma((8,)),
        ],
        compiler_params=pltpu.CompilerParams(vmem_limit_bytes=32 * 1024 * 1024, collective_id=layer, has_side_effects=True),
        cost_estimate=pl.CostEstimate(flops=200000000, bytes_accessed=8000000, transcendentals=0),
        name=f"mlp{layer}",
    )(x, gain, wg, wu, wd)


def solution(mesh):
    row_spec = P(("replica", "dp"), None)
    len_spec = P(("replica", "dp"))
    cache_spec = P(("replica", "dp"), None, None)
    in_specs = (row_spec, len_spec, cache_spec, cache_spec) + (P(),) * 13
    out_specs = (P("replica", None), cache_spec, cache_spec)

    def device_step(x_rows, lengths, cache0, cache1, attn_gain, w_dkv, kv_gain, wq_a, q_gain, wq_b, w_uk, w_uv, w_o, ffn_gain, w_gate, w_up, w_down):
        half = ROPE // 2
        inv_freq = 10000.0 ** (-(np.arange(128) % half) / half)
        freq = jnp.asarray(inv_freq[None, :], F32)
        w_dkv = w_dkv.transpose(0, 2, 1)
        x = x_rows
        caches = []
        for layer, cache in enumerate((cache0, cache1)):
            x, c = attention(layer, lengths, x, freq, attn_gain, kv_gain, q_gain, cache.transpose(0, 2, 1), w_dkv, wq_a, wq_b, w_uk, w_uv, w_o)
            caches.append(c.transpose(0, 2, 1))
            x = mlp(layer, layer == 1, x, ffn_gain, w_gate, w_up, w_down)
        return x.reshape(-1, DIM), caches[0], caches[1]

    return jax.shard_map(device_step, mesh=mesh, in_specs=in_specs, out_specs=out_specs, check_vma=False)
```

```python
import functools

import jax
import jax.numpy as jnp
import numpy as np
from jax import lax
from jax.experimental import pallas as pl
from jax.experimental.pallas import tpu as pltpu
from jax.sharding import PartitionSpec as P

BF = jnp.bfloat16
F32 = jnp.float32
MESH = pl.DeviceIdType.MESH
NT = (((1,), (1,)), ((), ()))

SEQ = 1024
DIM = 2048
FFN = 10240
HEADS = 20
KVR = 512
NOPE = 192
ROPE = 64
QKD = NOPE + ROPE
CACHE = KVR + ROPE
QR = 768
VD = 256
ROWS = 2
PAD = 16
HP = 32
GROUP = 16
FS = FFN // GROUP
QB = 4
KC = 512
WOC = HEADS * VD // KC
AHEAD = 13


def rms(v, gain):
    return v * lax.rsqrt(jnp.mean(v * v, axis=-1, keepdims=True) + 1e-6) * gain


def rope_lanes(t, cos_t, sin_t):
    lane = lax.broadcasted_iota(jnp.int32, t.shape, 1)
    swapped = jnp.where(lane < ROPE // 2, pltpu.roll(t, 128 - ROPE // 2, 1), pltpu.roll(t, ROPE // 2, 1))
    return t * cos_t + swapped * sin_t


def dev(i):
    return (lax.axis_index("replica"), i)


def remote(src, dst, send_sem, recv_sem, peer):
    return pltpu.make_async_remote_copy(src_ref=src, dst_ref=dst, send_sem=send_sem, recv_sem=recv_sem, device_id=dev(peer), device_id_type=MESH)


def step_kernel(len_ref, x_ref, freq_ref, ag_ref, kvg_ref, qg_ref, fg_ref, cache0_ref, cache1_ref, wdkv_ref, wqa_ref, wqb_ref, wuk_ref, wuv_ref, wo_ref, wg_ref, wu_ref, wd_ref,
                out_ref, ne_ref,
                wdkv, wqa, wqb, wuk, wuv, wo, cbuf, wg, wu, wd, xs, ks, qf, qlat, qrs, of, ob, acc, xm, xg, xf, pf, ps, pr, ps2, pr2, fb,
                sems, s1, r1, s2, r2, fs, fr, ds, dr, os_):
    idx = lax.axis_index("dp")
    core = lax.rem(idx, 2)
    cx = lax.rem(lax.div(idx, 2), 4)
    cy = lax.rem(lax.div(idx, 8), 4)
    cz = lax.div(idx, 32)
    gx, gy, gz = lax.div(cx, 2), lax.div(cy, 2), lax.div(cz, 2)
    bx, by, bz = lax.rem(cx, 2), lax.rem(cy, 2), lax.rem(cz, 2)
    chip = bz * 4 + by * 2 + bx
    me = chip * 2 + core

    def index(z, y, x, c):
        return z * 32 + y * 8 + x * 2 + c

    def flip(m):
        z = lax.rem(bz + m // 8, 2)
        y = lax.rem(by + m // 4 % 2, 2)
        x = lax.rem(bx + m // 2 % 2, 2)
        c = lax.rem(core + m % 2, 2)
        return z * 8 + y * 4 + x * 2 + c, index(gz * 2 + z, gy * 2 + y, gx * 2 + x, c)

    def away(k):
        return index(lax.rem(cz + lax.div(k, 16), 4), lax.rem(cy + lax.rem(lax.div(k, 4), 4), 4), lax.rem(cx + lax.rem(k, 4), 4), core)

    barrier = pltpu.get_barrier_semaphore()

    def greet(k, carry):
        pl.semaphore_signal(barrier, inc=1, device_id=dev(away(k)), device_id_type=MESH)
        return carry

    lax.fori_loop(1, 64, greet, 0)
    for m in range(1, GROUP, 2):
        pl.semaphore_signal(barrier, inc=1, device_id=dev(flip(m)[1]), device_id_type=MESH)

    half = HEADS // 2
    qc = HEADS * QKD // QB
    mine = pl.ds(pl.multiple_of(me * FS, FS), FS)

    def loads_of(layer):
        chunks = [(wdkv_ref.at[layer], wdkv), (wqa_ref.at[layer], wqa)]
        chunks += [(wqb_ref.at[layer, :, pl.ds(i * qc, qc)], wqb.at[:, pl.ds(i * qc, qc)]) for i in range(QB)]
        chunks += [(wuk_ref.at[layer, pl.ds(i * half, half)], wuk.at[pl.ds(i * half, half)]) for i in range(2)]
        chunks += [((cache0_ref, cache1_ref)[layer], cbuf)]
        chunks += [(wuv_ref.at[layer, pl.ds(i * half, half)], wuv.at[pl.ds(i * half, half)]) for i in range(2)]
        chunks += [(wo_ref.at[layer, pl.ds(i * KC, KC)], wo.at[pl.ds(i * KC, KC)]) for i in range(WOC)]
        chunks += [(wg_ref.at[layer, :, mine], wg), (wu_ref.at[layer, :, mine], wu), (wd_ref.at[layer, mine, :], wd)]
        return [pltpu.make_async_copy(s, d, sems.at[i]) for i, (s, d) in enumerate(chunks)]

    first_uv = 5 + QB
    first_wo = first_uv + 2
    first_mlp = first_wo + WOC
    loads = [loads_of(0), loads_of(1)]
    for cp in loads[0][:AHEAD]:
        cp.start()

    lane16 = lax.broadcasted_iota(jnp.int32, (PAD, 128), 1)
    row16 = lax.broadcasted_iota(jnp.int32, (PAD, 128), 0)
    angle = jnp.where(row16 == 0, len_ref[0], len_ref[1]).astype(F32) * freq_ref[...]
    cos_t = jnp.where(lane16 < ROPE, jnp.cos(angle), 0.0)
    sin_t = jnp.sin(angle)
    sin_t = jnp.where(lane16 < ROPE, jnp.where(lane16 < ROPE // 2, -sin_t, sin_t), 0.0)

    xs[...] = jnp.zeros_like(xs)
    xs[0:ROWS, :] = x_ref[...].astype(F32)
    ks[...] = jnp.zeros_like(ks)
    of[...] = jnp.zeros_like(of)
    for b in range(ROWS):
        qlat[b, 16:HP, :] = jnp.zeros((HP - 16, KVR), F32)
        qrs[b, 16:HP, :] = jnp.zeros((HP - 16, 128), F32)

    def attention(layer):
        def ready(i):
            loads[layer][i].wait()
            if layer == 0 and i + AHEAD < len(loads[0]):
                loads[0][i + AHEAD].start()

        h = rms(xs[...], ag_ref[layer:layer + 1, :]).astype(BF)
        ready(0)
        k = lax.dot_general(h, wdkv[...], NT, preferred_element_type=F32)
        ready(1)
        qa = jnp.dot(h, wqa[...], preferred_element_type=F32)
        qa = rms(qa, qg_ref[layer:layer + 1, :]).astype(BF)
        ks[:, 0:CACHE] = k
        ks[:, 0:KVR] = rms(k[:, 0:KVR], kvg_ref[layer:layer + 1, :]).astype(BF).astype(F32)
        ks[:, KVR:KVR + 128] = rope_lanes(ks[:, KVR:KVR + 128], cos_t, sin_t).astype(BF).astype(F32)
        ne_ref[layer] = ks[0:ROWS, 0:CACHE].astype(BF)

        heads_q = HEADS // QB
        qparts = []
        for i in range(QB):
            ready(2 + i)
            qi = jnp.dot(qa, wqb[:, i * qc:(i + 1) * qc], preferred_element_type=F32).astype(BF)
            qf[:, i * qc:(i + 1) * qc] = qi.astype(F32)
            qparts.append(qi)
        for j in range(HEADS):
            if j % half == 0:
                ready(2 + QB + j // half)
            jj = j % heads_q
            qn = qparts[j // heads_q][:, jj * QKD:jj * QKD + NOPE]
            ql = jnp.dot(qn, wuk[j], preferred_element_type=F32)
            for b in range(ROWS):
                qlat[b, j:j + 1, :] = ql[b:b + 1, :]
                qrs[b, j:j + 1, :] = qf[b:b + 1, j * QKD + 128:(j + 1) * QKD]

        ready(4 + QB)
        ol = []
        slot = lax.broadcasted_iota(jnp.int32, (HP, SEQ), 1)
        for b in range(ROWS):
            p = len_ref[b]
            ql = qlat[b].astype(BF)
            qr = rope_lanes(pltpu.roll(qrs[b], 64, 1), cos_t[b:b + 1, :], sin_t[b:b + 1, :]).astype(BF)
            s = jnp.dot(ql, cbuf[b, 0:KVR, :], preferred_element_type=F32)
            s += jnp.dot(qr[:, 0:ROPE], cbuf[b, KVR:CACHE, :], preferred_element_type=F32)
            own = jnp.sum(ql.astype(F32) * ks[b:b + 1, 0:KVR], axis=-1, keepdims=True)
            own += jnp.sum(qr.astype(F32) * ks[b:b + 1, KVR:KVR + 128], axis=-1, keepdims=True)
            s = jnp.where(slot == p, own, s) * (QKD ** -0.5)
            s = jnp.where(slot <= p, s, -1e30)
            e = jnp.exp(s - jnp.max(s, axis=-1, keepdims=True))
            a = (e / jnp.sum(e, axis=-1, keepdims=True)).astype(BF)
            af = a.astype(F32)
            a_own = jnp.sum(jnp.where(slot == p, af, 0.0), axis=-1, keepdims=True)
            a_old = jnp.where(slot == p, 0.0, af).astype(BF)
            o = lax.dot_general(a_old, cbuf[b, 0:KVR, :], NT, preferred_element_type=F32)
            ol.append((o + a_own * ks[b:b + 1, 0:KVR]).astype(BF))
        olc = jnp.concatenate(ol, axis=0)
        for j in range(HEADS):
            if j % half == 0:
                ready(first_uv + j // half)
            r = jnp.dot(olc, wuv[j], preferred_element_type=F32)
            for b in range(ROWS):
                of[b:b + 1, j * VD:(j + 1) * VD] = r[b * HP + j:b * HP + j + 1, :]
        for i in range(WOC):
            ob[i] = of[:, i * KC:(i + 1) * KC].astype(BF)
        acc[...] = jnp.zeros_like(acc)

        def step(i, carry):
            at = pl.ds(pl.multiple_of(i * KC, KC), KC)
            pltpu.make_async_copy(wo_ref.at[layer, at], wo.at[at], sems.at[first_wo + i]).wait()
            acc[...] += jnp.dot(ob[i], wo[at, :], preferred_element_type=F32)
            return carry

        lax.fori_loop(0, WOC, step, 0)
        xm[layer] = (xs[0:ROWS, :] + acc[0:ROWS, :]).astype(BF)

    def group_rows(layer):
        copies = []
        for m in range(GROUP - 1, 0, -1):
            cp = remote(xm.at[layer], xg.at[me], s1.at[layer, m], r1.at[layer, m], flip(m)[1])
            cp.start()
            copies.append(cp)
        return copies

    def mlp_share(layer):
        xg[me] = xm[layer]
        for m in range(1, GROUP):
            r, peer = flip(m)
            remote(xm.at[layer], xg.at[r], s1.at[layer, m], r1.at[layer, m], peer).wait_recv()
        for d in range(GROUP):
            xf[ROWS * d:ROWS * (d + 1), :] = xg[d].astype(F32)
        g = rms(xf[...], fg_ref[layer:layer + 1, :]).astype(BF)
        loads[layer][first_mlp].wait()
        gate = jnp.dot(g, wg[...], preferred_element_type=F32)
        loads[layer][first_mlp + 1].wait()
        up = jnp.dot(g, wu[...], preferred_element_type=F32)
        u = (gate * jax.nn.sigmoid(gate) * up).astype(BF)
        loads[layer][first_mlp + 2].wait()
        pf[...] = jnp.dot(u, wd[...], preferred_element_type=F32)

    attention(0)
    pl.semaphore_wait(barrier, 63 + GROUP // 2)
    sent = group_rows(0)
    for cp in loads[1][:4 + QB]:
        cp.start()
    mlp_share(0)
    for d in range(GROUP):
        ps[d] = pf[ROWS * d:ROWS * (d + 1), :].astype(BF)
    for m in range(GROUP - 1, 0, -1):
        r, peer = flip(m)
        cp = remote(ps.at[r], pr.at[me], s2.at[0, m], r2.at[0, m], peer)
        cp.start()
        sent.append(cp)
    for cp in loads[1][4 + QB:]:
        cp.start()
    pr[me] = ps[me]
    for m in range(1, GROUP):
        r, peer = flip(m)
        remote(ps.at[r], pr.at[r], s2.at[0, m], r2.at[0, m], peer).wait_recv()
    total = pr[0].astype(F32)
    for d in range(1, GROUP):
        total += pr[d].astype(F32)
    xs[0:ROWS, :] = (xm[0].astype(F32) + total).astype(BF).astype(F32)

    attention(1)
    sent += group_rows(1)
    mlp_share(1)
    def cols(q, c):
        return pl.ds(pl.multiple_of(c * 1024 + q * 128, 128), 128)

    for d in range(GROUP):
        ps2[d] = pf[:, (d % 2) * 1024 + d // 2 * 128:(d % 2) * 1024 + d // 2 * 128 + 128].astype(BF)
    for m in range(GROUP - 1, 0, -1):
        r, peer = flip(m)
        cp = remote(ps2.at[r], pr2.at[me], s2.at[1, m], r2.at[1, m], peer)
        cp.start()
        sent.append(cp)
    pr2[me] = ps2[me]
    for m in range(1, GROUP):
        r, peer = flip(m)
        remote(ps2.at[r], pr2.at[r], s2.at[1, m], r2.at[1, m], peer).wait_recv()
    total = pr2[0].astype(F32)
    for d in range(1, GROUP):
        total += pr2[d].astype(F32)
    fin = (xf[:, cols(chip, core)] + total).astype(BF)
    for z in range(2):
        for y in range(2):
            fb[gz * 2 + z, gy * 2 + y, gx, :, cols(chip, core)] = fin[(z * 2 + y) * 8:(z * 2 + y) * 8 + 8, :]

    def block(ref, z, y, x, c):
        q = lax.rem(z, 2) * 4 + lax.rem(y, 2) * 2 + lax.rem(x, 2)
        return ref.at[pl.ds(lax.div(z, 2) * 2, 2), pl.ds(lax.div(y, 2) * 2, 2), lax.div(x, 2), :, cols(q, c)]

    def side(ref, z, y, x, c):
        return ref.at[pl.ds(z * 2, 2), pl.ds(y * 2, 2), x, :, pl.ds(pl.multiple_of(c * 1024, 1024), 1024)]

    own_block = block(fb, cz, cy, cx, core)

    def digit(a):
        return lax.rem(2 + 3 * a, 4)

    def spread(i, carry):
        k = digit(lax.div(i, 16)) * 16 + digit(lax.rem(lax.div(i, 4), 4)) * 4 + digit(lax.rem(i, 4))

        @pl.when(k != 0)
        def _():
            remote(own_block, own_block, fs.at[k], fr.at[k], away(k)).start()
        return carry

    lax.fori_loop(0, 64, spread, 0)
    partner = index(cz, cy, cx, 1 - core)

    def gathered(t, carry):
        z = lax.rem(gz + lax.div(t, 4), 2)
        y = lax.rem(gy + lax.rem(lax.div(t, 2), 2), 2)
        x = lax.rem(gx + lax.rem(t, 2), 2)

        def arrive(q, carry):
            oz, oy, ox = z * 2 + lax.div(q, 4), y * 2 + lax.rem(lax.div(q, 2), 2), x * 2 + lax.rem(q, 2)
            k = lax.rem(cz + 4 - oz, 4) * 16 + lax.rem(cy + 4 - oy, 4) * 4 + lax.rem(cx + 4 - ox, 4)

            @pl.when(k != 0)
            def _():
                remote(own_block, block(fb, oz, oy, ox, core), fs.at[k], fr.at[k], index(oz, oy, ox, core)).wait_recv()
            return carry

        lax.fori_loop(0, 8, arrive, 0)
        part = side(fb, z, y, x, core)
        remote(part, part, ds.at[t], dr.at[t], partner).start()
        pltpu.make_async_copy(part, side(out_ref, z, y, x, core), os_.at[t]).start()
        return carry

    lax.fori_loop(0, 8, gathered, 0)

    def passed(t, carry):
        z = lax.rem(gz + lax.div(t, 4), 2)
        y = lax.rem(gy + lax.rem(lax.div(t, 2), 2), 2)
        x = lax.rem(gx + lax.rem(t, 2), 2)
        part = side(fb, z, y, x, 1 - core)
        remote(part, part, ds.at[t], dr.at[t], partner).wait_recv()
        pltpu.make_async_copy(part, side(out_ref, z, y, x, 1 - core), os_.at[8 + t]).start()
        return carry

    lax.fori_loop(0, 8, passed, 0)
    for cp in sent:
        cp.wait_send()

    def sent_block(k, carry):
        remote(own_block, own_block, fs.at[k], fr.at[k], away(k)).wait_send()
        return carry

    lax.fori_loop(1, 64, sent_block, 0)

    def finish(t, carry):
        part = side(fb, 0, 0, 0, core)
        remote(part, part, ds.at[t], dr.at[t], partner).wait_send()
        pltpu.make_async_copy(part, side(out_ref, 0, 0, 0, core), os_.at[t]).wait()
        pltpu.make_async_copy(part, side(out_ref, 0, 0, 0, core), os_.at[8 + t]).wait()
        return carry

    lax.fori_loop(0, 8, finish, 0)


def two_layers(lengths, x, freq, ag, kvg, qg, fg, cache0, cache1, wdkv, wqa, wqb, wuk, wuv, wo, wg, wu, wd):
    vm = pl.BlockSpec(memory_space=pltpu.VMEM)
    anyspec = pl.BlockSpec(memory_space=pl.ANY)
    dma = pltpu.SemaphoreType.DMA
    n_loads = 5 + QB + 2 + WOC + 3
    return pl.pallas_call(
        step_kernel,
        out_shape=(jax.ShapeDtypeStruct((4, 4, 2, 8, DIM), BF), jax.ShapeDtypeStruct((2, ROWS, CACHE), BF)),
        in_specs=[pl.BlockSpec(memory_space=pltpu.SMEM)] + [vm] * 6 + [anyspec] * 11,
        out_specs=(anyspec, vm),
        scratch_shapes=[
            pltpu.VMEM((CACHE, DIM), BF), pltpu.VMEM((DIM, QR), BF), pltpu.VMEM((QR, HEADS * QKD), BF),
            pltpu.VMEM((HEADS, NOPE, KVR), BF), pltpu.VMEM((HEADS, KVR, VD), BF), pltpu.VMEM((HEADS * VD, DIM), BF),
            pltpu.VMEM((ROWS, CACHE, SEQ), BF),
            pltpu.VMEM((DIM, FS), BF), pltpu.VMEM((DIM, FS), BF), pltpu.VMEM((FS, DIM), BF),
            pltpu.VMEM((PAD, DIM), F32), pltpu.VMEM((PAD, KVR + 128), F32),
            pltpu.VMEM((PAD, HEADS * QKD), F32), pltpu.VMEM((ROWS, HP, KVR), F32), pltpu.VMEM((ROWS, HP, 128), F32),
            pltpu.VMEM((PAD, HEADS * VD), F32), pltpu.VMEM((WOC, PAD, KC), BF), pltpu.VMEM((PAD, DIM), F32),
            pltpu.VMEM((2, ROWS, DIM), BF), pltpu.VMEM((GROUP, ROWS, DIM), BF), pltpu.VMEM((GROUP * ROWS, DIM), F32),
            pltpu.VMEM((GROUP * ROWS, DIM), F32), pltpu.VMEM((GROUP, ROWS, DIM), BF), pltpu.VMEM((GROUP, ROWS, DIM), BF),
            pltpu.VMEM((GROUP, GROUP * ROWS, 128), BF), pltpu.VMEM((GROUP, GROUP * ROWS, 128), BF),
            pltpu.VMEM((4, 4, 2, 8, DIM), BF),
            dma((n_loads,)), dma((2, GROUP)), dma((2, GROUP)), dma((2, GROUP)), dma((2, GROUP)),
            dma((64,)), dma((64,)), dma((8,)), dma((8,)), dma((16,)),
        ],
        compiler_params=pltpu.CompilerParams(vmem_limit_bytes=62 * 1024 * 1024, collective_id=0, has_side_effects=True),
        name="two_layers",
    )(lengths, x, freq, ag, kvg, qg, fg, cache0, cache1, wdkv, wqa, wqb, wuk, wuv, wo, wg, wu, wd)


def solution(mesh):
    row_spec = P(("replica", "dp"), None)
    len_spec = P(("replica", "dp"))
    cache_spec = P(("replica", "dp"), None, None)
    in_specs = (row_spec, len_spec, cache_spec, cache_spec) + (P(),) * 13
    out_specs = (P("replica", None), cache_spec, cache_spec)

    def device_step(x_rows, lengths, cache0, cache1, attn_gain, w_dkv, kv_gain, wq_a, q_gain, wq_b, w_uk, w_uv, w_o, ffn_gain, w_gate, w_up, w_down):
        half = ROPE // 2
        inv_freq = 10000.0 ** (-(np.arange(128) % half) / half)
        freq = jnp.asarray(inv_freq[None, :], F32)
        x, ne = two_layers(lengths, x_rows, freq, attn_gain, kv_gain, q_gain, ffn_gain, cache0.transpose(0, 2, 1), cache1.transpose(0, 2, 1),
                           w_dkv.transpose(0, 2, 1), wq_a, wq_b, w_uk, w_uv, w_o, w_gate, w_up, w_down)
        at_slot = lax.broadcasted_iota(jnp.int32, (1, SEQ), 1) == lengths[:, None]
        caches = [jnp.where(at_slot[:, :, None], ne[layer][:, None, :], cache) for layer, cache in enumerate((cache0, cache1))]
        return x.reshape(-1, DIM), caches[0], caches[1]

    return jax.shard_map(device_step, mesh=mesh, in_specs=in_specs, out_specs=out_specs, check_vma=False)
```

```python
import functools

import jax
import jax.numpy as jnp
import numpy as np
from jax import lax
from jax.experimental import pallas as pl
from jax.experimental.pallas import tpu as pltpu
from jax.sharding import PartitionSpec as P

BF = jnp.bfloat16
F32 = jnp.float32
MESH = pl.DeviceIdType.MESH
NT = (((1,), (1,)), ((), ()))

SEQ = 1024
DIM = 2048
FFN = 10240
HEADS = 20
KVR = 512
NOPE = 192
ROPE = 64
QKD = NOPE + ROPE
CACHE = KVR + ROPE
QR = 768
VD = 256
ROWS = 2
PAD = 16
HP = 32
GROUP = 16
HALF = DIM // 2
FS = FFN // GROUP
QB = 4
KC = 1024
WOC = HEADS * VD // KC
AHEAD = 12


AT_X, AT_AG, AT_FG, AT_KV = 0, DIM, 2 * DIM, 3 * DIM
AT_QG = AT_KV + KVR
AT_FREQ = AT_QG + QR
AT_LEN = AT_FREQ + 128


def rms(v, gain):
    return v * lax.rsqrt(jnp.mean(v * v, axis=-1, keepdims=True) + 1e-6) * gain


def rope_lanes(t, cos_t, sin_t):
    lane = lax.broadcasted_iota(jnp.int32, t.shape, 1)
    swapped = jnp.where(lane < ROPE // 2, pltpu.roll(t, 128 - ROPE // 2, 1), pltpu.roll(t, ROPE // 2, 1))
    return t * cos_t + swapped * sin_t


def dev(i):
    return (lax.axis_index("replica"), i)


def remote(src, dst, send_sem, recv_sem, peer):
    return pltpu.make_async_remote_copy(src_ref=src, dst_ref=dst, send_sem=send_sem, recv_sem=recv_sem, device_id=dev(peer), device_id_type=MESH)


def step_kernel(pk_ref, cache0_ref, cache1_ref, wdkv_ref, wqa_ref, wqb_ref, wuk_ref, wuv_ref, wo_ref, wg_ref, wu_ref, wd_ref,
                out_ref, keep0, keep1,
                wdkv, wqa, wqb, wuk, wuv, wo, wg, wu, wd, xs, ks, qf, qlat, qrs, of, ob, acc, entry, osend, orecv, xpart, xsend, xm, xg, xf, pf, ps, pr, ps2, pr2, fb,
                sems, s1, r1, s2, r2, p1, q1, fs, fr, ds, dr, os_):
    idx = lax.axis_index("dp")
    core = lax.rem(idx, 2)
    cx = lax.rem(lax.div(idx, 2), 4)
    cy = lax.rem(lax.div(idx, 8), 4)
    cz = lax.div(idx, 32)
    gx, gy, gz = lax.div(cx, 2), lax.div(cy, 2), lax.div(cz, 2)
    bx, by, bz = lax.rem(cx, 2), lax.rem(cy, 2), lax.rem(cz, 2)
    chip = bz * 4 + by * 2 + bx
    me = chip * 2 + core

    def index(z, y, x, c):
        return z * 32 + y * 8 + x * 2 + c

    def flip(m):
        z = lax.rem(bz + m // 8, 2)
        y = lax.rem(by + m // 4 % 2, 2)
        x = lax.rem(bx + m // 2 % 2, 2)
        c = lax.rem(core + m % 2, 2)
        return z * 8 + y * 4 + x * 2 + c, index(gz * 2 + z, gy * 2 + y, gx * 2 + x, c)

    def away(k):
        return index(lax.rem(cz + lax.div(k, 16), 4), lax.rem(cy + lax.rem(lax.div(k, 4), 4), 4), lax.rem(cx + lax.rem(k, 4), 4), core)

    half = HEADS // 2
    qc = HEADS * QKD // QB
    mine = pl.ds(pl.multiple_of(me * FS, FS), FS)
    my_half = pl.ds(pl.multiple_of(core * HALF, HALF), HALF)
    its_half = pl.ds(pl.multiple_of((1 - core) * HALF, HALF), HALF)
    partner = index(cz, cy, cx, 1 - core)

    def loads_of(layer):
        chunks = [(wdkv_ref.at[layer], wdkv), (wqa_ref.at[layer], wqa)]
        chunks += [(wqb_ref.at[layer, :, pl.ds(i * qc, qc)], wqb.at[:, pl.ds(i * qc, qc)]) for i in range(QB)]
        chunks += [(wuk_ref.at[layer, pl.ds(i * half, half)], wuk.at[pl.ds(i * half, half)]) for i in range(2)]
        chunks += [((cache0_ref, cache1_ref)[layer], (keep0, keep1)[layer])]
        chunks += [(wuv_ref.at[layer, pl.ds(i * half, half)], wuv.at[pl.ds(i * half, half)]) for i in range(2)]
        chunks += [(wo_ref.at[layer, pl.ds(i * KC, KC), my_half], wo.at[pl.ds(i * KC, KC)]) for i in range(WOC)]
        chunks += [(wg_ref.at[layer, :, mine], wg), (wu_ref.at[layer, :, mine], wu), (wd_ref.at[layer, mine, :], wd)]
        return [pltpu.make_async_copy(s, d, sems.at[i]) for i, (s, d) in enumerate(chunks)]

    first_uv = 5 + QB
    first_wo = first_uv + 2
    first_mlp = first_wo + WOC
    loads = [loads_of(0), loads_of(1)]
    for cp in loads[0][:AHEAD]:
        cp.start()

    barrier = pltpu.get_barrier_semaphore()

    def greet(k, carry):
        pl.semaphore_signal(barrier, inc=1, device_id=dev(away(k)), device_id_type=MESH)
        return carry

    lax.fori_loop(1, 64, greet, 0)
    for m in range(1, GROUP, 2):
        pl.semaphore_signal(barrier, inc=1, device_id=dev(flip(m)[1]), device_id_type=MESH)


    lane16 = lax.broadcasted_iota(jnp.int32, (PAD, 128), 1)
    row16 = lax.broadcasted_iota(jnp.int32, (PAD, 128), 0)
    at_len = [pk_ref[b:b + 1, AT_LEN:AT_LEN + SEQ].astype(jnp.int32) for b in range(ROWS)]
    angle = jnp.where(row16 == 0, pk_ref[0:1, AT_LEN:AT_LEN + 128], pk_ref[1:2, AT_LEN:AT_LEN + 128]) * pk_ref[0:1, AT_FREQ:AT_FREQ + 128]
    cos_t = jnp.where(lane16 < ROPE, jnp.cos(angle), 0.0)
    sin_t = jnp.sin(angle)
    sin_t = jnp.where(lane16 < ROPE, jnp.where(lane16 < ROPE // 2, -sin_t, sin_t), 0.0)

    xs[...] = jnp.zeros_like(xs)
    xs[0:ROWS, :] = pk_ref[:, AT_X:AT_X + DIM]
    xsend[0] = pk_ref[:, AT_X:AT_X + DIM].astype(BF)
    ks[...] = jnp.zeros_like(ks)
    of[...] = jnp.zeros_like(of)
    for b in range(ROWS):
        qlat[b, 16:HP, :] = jnp.zeros((HP - 16, KVR), F32)
        qrs[b, 16:HP, :] = jnp.zeros((HP - 16, 128), F32)

    def attention(layer):
        cbuf = (keep0, keep1)[layer]

        def ready(i):
            loads[layer][i].wait()
            if layer == 0 and i + AHEAD < len(loads[0]):
                loads[0][i + AHEAD].start()

        h = rms(xs[...], pk_ref[layer:layer + 1, AT_AG:AT_AG + DIM]).astype(BF)
        ready(0)
        k = lax.dot_general(h, wdkv[...], NT, preferred_element_type=F32)
        ready(1)
        qa = jnp.dot(h, wqa[...], preferred_element_type=F32)
        qa = rms(qa, pk_ref[layer:layer + 1, AT_QG:AT_QG + QR]).astype(BF)
        ks[:, 0:CACHE] = k
        ks[:, 0:KVR] = rms(k[:, 0:KVR], pk_ref[layer:layer + 1, AT_KV:AT_KV + KVR]).astype(BF).astype(F32)
        ks[:, KVR:KVR + 128] = rope_lanes(ks[:, KVR:KVR + 128], cos_t, sin_t).astype(BF).astype(F32)
        entry[layer] = ks[:, 0:CACHE].astype(BF)

        heads_q = HEADS // QB
        qparts = []
        for i in range(QB):
            ready(2 + i)
            qi = jnp.dot(qa, wqb[:, i * qc:(i + 1) * qc], preferred_element_type=F32).astype(BF)
            qf[:, i * qc:(i + 1) * qc] = qi.astype(F32)
            qparts.append(qi)
        for j in range(HEADS):
            if j % half == 0:
                ready(2 + QB + j // half)
            jj = j % heads_q
            qn = qparts[j // heads_q][:, jj * QKD:jj * QKD + NOPE]
            ql = jnp.dot(qn, wuk[j], preferred_element_type=F32)
            for b in range(ROWS):
                qlat[b, j:j + 1, :] = ql[b:b + 1, :]
                qrs[b, j:j + 1, :] = qf[b:b + 1, j * QKD + 128:(j + 1) * QKD]

        ready(4 + QB)
        ol = []
        slot = lax.broadcasted_iota(jnp.int32, (HP, SEQ), 1)
        for b in range(ROWS):
            p = at_len[b]
            ql = qlat[b].astype(BF)
            qr = rope_lanes(pltpu.roll(qrs[b], 64, 1), cos_t[b:b + 1, :], sin_t[b:b + 1, :]).astype(BF)
            s = jnp.dot(ql, cbuf[b, 0:KVR, :], preferred_element_type=F32)
            s += jnp.dot(qr[:, 0:ROPE], cbuf[b, KVR:CACHE, :], preferred_element_type=F32)
            own = jnp.sum(ql.astype(F32) * ks[b:b + 1, 0:KVR], axis=-1, keepdims=True)
            own += jnp.sum(qr.astype(F32) * ks[b:b + 1, KVR:KVR + 128], axis=-1, keepdims=True)
            s = jnp.where(slot == p, own, s) * (QKD ** -0.5)
            s = jnp.where(slot <= p, s, -1e30)
            e = jnp.exp(s - jnp.max(s, axis=-1, keepdims=True))
            a = (e / jnp.sum(e, axis=-1, keepdims=True)).astype(BF)
            af = a.astype(F32)
            a_own = jnp.sum(jnp.where(slot == p, af, 0.0), axis=-1, keepdims=True)
            a_old = jnp.where(slot == p, 0.0, af).astype(BF)
            o = lax.dot_general(a_old, cbuf[b, 0:KVR, :], NT, preferred_element_type=F32)
            ol.append((o + a_own * ks[b:b + 1, 0:KVR]).astype(BF))
        olc = jnp.concatenate(ol, axis=0)
        for j in range(HEADS):
            if j % half == 0:
                ready(first_uv + j // half)
            r = jnp.dot(olc, wuv[j], preferred_element_type=F32)
            for b in range(ROWS):
                of[b:b + 1, j * VD:(j + 1) * VD] = r[b * HP + j:b * HP + j + 1, :]
        osend[layer] = of[0:ROWS, :].astype(BF)
        acc[...] = jnp.zeros_like(acc)
        if layer == 0:
            pl.semaphore_wait(barrier, 63 + GROUP // 2)
            cp = remote(xsend.at[0], xpart.at[0], p1.at[0, 1], q1.at[0, 1], partner)
            cp.start()
            sent.append(cp)
        cp = remote(osend.at[layer], orecv.at[layer], p1.at[layer, 0], q1.at[layer, 0], partner)
        cp.start()
        sent.append(cp)
        cp.wait_recv()
        of[ROWS:2 * ROWS, :] = orecv[layer].astype(F32)
        for i in range(WOC):
            ob[i] = of[:, i * KC:(i + 1) * KC].astype(BF)

        def step(i, carry):
            at = pl.ds(pl.multiple_of(i * KC, KC), KC)
            pltpu.make_async_copy(wo_ref.at[layer, at, my_half], wo.at[at], sems.at[first_wo + i]).wait()
            acc[...] += jnp.dot(ob[i], wo[at, :], preferred_element_type=F32)
            return carry

        lax.fori_loop(0, WOC, step, 0)
        remote(xpart.at[layer], xpart.at[layer], p1.at[layer, 1], q1.at[layer, 1], partner).wait_recv()
        xm[layer, 0:ROWS, :] = (xs[0:ROWS, my_half] + acc[0:ROWS, :]).astype(BF)
        xm[layer, ROWS:2 * ROWS, :] = (xpart[layer, :, my_half].astype(F32) + acc[ROWS:2 * ROWS, :]).astype(BF)

    def insert(layer):
        keep = (keep0, keep1)[layer]

        def tile(t, carry):
            at = pl.ds(pl.multiple_of(t * 128, 128), 128)
            lane = lax.broadcasted_iota(jnp.int32, (CACHE, 128), 1) + t * 128
            for b in range(ROWS):
                hot = jnp.where((row16 == b) & (lane16 + t * 128 == at_len[b][:, 0:128]), 1.0, 0.0).astype(BF)
                col = lax.dot_general(entry[layer], hot, (((0,), (0,)), ((), ())), preferred_element_type=F32)
                keep[b, :, at] = jnp.where(lane == at_len[b][:, 0:128], col, keep[b, :, at].astype(F32)).astype(BF)
            return carry

        lax.fori_loop(0, SEQ // 128, tile, 0)

    def group_rows(layer):
        copies = []
        for m in range(GROUP - 1, 0, -1):
            cp = remote(xm.at[layer], xg.at[me], s1.at[layer, m], r1.at[layer, m], flip(m)[1])
            cp.start()
            copies.append(cp)
        return copies

    def mlp_share(layer):
        xg[me] = xm[layer]
        for m in range(1, GROUP):
            r, peer = flip(m)
            remote(xm.at[layer], xg.at[r], s1.at[layer, m], r1.at[layer, m], peer).wait_recv()
        for d in range(GROUP):
            at = pl.ds(d % 2 * HALF, HALF)
            xf[ROWS * d:ROWS * (d + 1), at] = xg[d, 0:ROWS, :].astype(F32)
            d2 = d + 1 - 2 * (d % 2)
            xf[ROWS * d2:ROWS * (d2 + 1), at] = xg[d, ROWS:2 * ROWS, :].astype(F32)
        g = rms(xf[...], pk_ref[layer:layer + 1, AT_FG:AT_FG + DIM]).astype(BF)
        loads[layer][first_mlp].wait()
        gate = jnp.dot(g, wg[...], preferred_element_type=F32)
        loads[layer][first_mlp + 1].wait()
        up = jnp.dot(g, wu[...], preferred_element_type=F32)
        u = (gate * jax.nn.sigmoid(gate) * up).astype(BF)
        loads[layer][first_mlp + 2].wait()
        pf[...] = jnp.dot(u, wd[...], preferred_element_type=F32)

    sent = []
    attention(0)
    sent += group_rows(0)
    for cp in loads[1][:4 + QB]:
        cp.start()
    mlp_share(0)
    for d in range(GROUP):
        ps[d] = pf[ROWS * d:ROWS * (d + 1), :].astype(BF)
    for m in range(GROUP - 1, 0, -1):
        r, peer = flip(m)
        cp = remote(ps.at[r], pr.at[me], s2.at[0, m], r2.at[0, m], peer)
        cp.start()
        sent.append(cp)
    for cp in loads[1][4 + QB:]:
        cp.start()
    pr[me] = ps[me]
    insert(0)
    for m in range(1, GROUP):
        r, peer = flip(m)
        remote(ps.at[r], pr.at[r], s2.at[0, m], r2.at[0, m], peer).wait_recv()
    total = pr[0].astype(F32)
    for d in range(1, GROUP):
        total += pr[d].astype(F32)
    xs[0:ROWS, my_half] = xg[me, 0:ROWS, :].astype(F32)
    xs[0:ROWS, its_half] = xg[me + 1 - 2 * core, ROWS:2 * ROWS, :].astype(F32)
    new_x = (xs[0:ROWS, :] + total).astype(BF)
    xsend[1] = new_x
    xs[0:ROWS, :] = new_x.astype(F32)
    cp = remote(xsend.at[1], xpart.at[1], p1.at[1, 1], q1.at[1, 1], partner)
    cp.start()
    sent.append(cp)

    attention(1)
    sent += group_rows(1)
    mlp_share(1)
    def cols(q, c):
        return pl.ds(pl.multiple_of(c * 1024 + q * 128, 128), 128)

    for d in range(GROUP):
        ps2[d] = pf[:, (d % 2) * 1024 + d // 2 * 128:(d % 2) * 1024 + d // 2 * 128 + 128].astype(BF)
    for m in range(GROUP - 1, 0, -1):
        r, peer = flip(m)
        cp = remote(ps2.at[r], pr2.at[me], s2.at[1, m], r2.at[1, m], peer)
        cp.start()
        sent.append(cp)
    pr2[me] = ps2[me]
    for m in range(1, GROUP):
        r, peer = flip(m)
        remote(ps2.at[r], pr2.at[r], s2.at[1, m], r2.at[1, m], peer).wait_recv()
    total = pr2[0].astype(F32)
    for d in range(1, GROUP):
        total += pr2[d].astype(F32)
    fin = (xf[:, cols(chip, core)] + total).astype(BF)
    for z in range(2):
        for y in range(2):
            fb[gz * 2 + z, gy * 2 + y, gx, :, cols(chip, core)] = fin[(z * 2 + y) * 8:(z * 2 + y) * 8 + 8, :]

    def block(ref, z, y, x, c):
        q = lax.rem(z, 2) * 4 + lax.rem(y, 2) * 2 + lax.rem(x, 2)
        return ref.at[pl.ds(lax.div(z, 2) * 2, 2), pl.ds(lax.div(y, 2) * 2, 2), lax.div(x, 2), :, cols(q, c)]

    def side(ref, z, y, x, c):
        return ref.at[pl.ds(z * 2, 2), pl.ds(y * 2, 2), x, :, pl.ds(pl.multiple_of(c * 1024, 1024), 1024)]

    own_block = block(fb, cz, cy, cx, core)

    def digit(a):
        return lax.rem(2 + 3 * a, 4)

    def spread(i, carry):
        k = digit(lax.div(i, 16)) * 16 + digit(lax.rem(lax.div(i, 4), 4)) * 4 + digit(lax.rem(i, 4))

        @pl.when(k != 0)
        def _():
            remote(own_block, own_block, fs.at[k], fr.at[k], away(k)).start()
        return carry

    lax.fori_loop(0, 64, spread, 0)
    insert(1)

    def gathered(t, carry):
        z = lax.rem(gz + lax.div(t, 4), 2)
        y = lax.rem(gy + lax.rem(lax.div(t, 2), 2), 2)
        x = lax.rem(gx + lax.rem(t, 2), 2)

        def arrive(q, carry):
            oz, oy, ox = z * 2 + lax.div(q, 4), y * 2 + lax.rem(lax.div(q, 2), 2), x * 2 + lax.rem(q, 2)
            k = lax.rem(cz + 4 - oz, 4) * 16 + lax.rem(cy + 4 - oy, 4) * 4 + lax.rem(cx + 4 - ox, 4)

            @pl.when(k != 0)
            def _():
                remote(own_block, block(fb, oz, oy, ox, core), fs.at[k], fr.at[k], index(oz, oy, ox, core)).wait_recv()
            return carry

        lax.fori_loop(0, 8, arrive, 0)
        part = side(fb, z, y, x, core)
        remote(part, part, ds.at[t], dr.at[t], partner).start()
        pltpu.make_async_copy(part, side(out_ref, z, y, x, core), os_.at[t]).start()
        return carry

    lax.fori_loop(0, 8, gathered, 0)

    def passed(t, carry):
        z = lax.rem(gz + lax.div(t, 4), 2)
        y = lax.rem(gy + lax.rem(lax.div(t, 2), 2), 2)
        x = lax.rem(gx + lax.rem(t, 2), 2)
        part = side(fb, z, y, x, 1 - core)
        remote(part, part, ds.at[t], dr.at[t], partner).wait_recv()
        pltpu.make_async_copy(part, side(out_ref, z, y, x, 1 - core), os_.at[8 + t]).start()
        return carry

    lax.fori_loop(0, 8, passed, 0)
    for cp in sent:
        cp.wait_send()

    def sent_block(k, carry):
        remote(own_block, own_block, fs.at[k], fr.at[k], away(k)).wait_send()
        return carry

    lax.fori_loop(1, 64, sent_block, 0)

    def finish(t, carry):
        part = side(fb, 0, 0, 0, core)
        remote(part, part, ds.at[t], dr.at[t], partner).wait_send()
        pltpu.make_async_copy(part, side(out_ref, 0, 0, 0, core), os_.at[t]).wait()
        pltpu.make_async_copy(part, side(out_ref, 0, 0, 0, core), os_.at[8 + t]).wait()
        return carry

    lax.fori_loop(0, 8, finish, 0)


def two_layers(pk, cache0, cache1, wdkv, wqa, wqb, wuk, wuv, wo, wg, wu, wd):
    vm = pl.BlockSpec(memory_space=pltpu.VMEM)
    anyspec = pl.BlockSpec(memory_space=pl.ANY)
    dma = pltpu.SemaphoreType.DMA
    n_loads = 5 + QB + 2 + WOC + 3
    return pl.pallas_call(
        step_kernel,
        out_shape=(jax.ShapeDtypeStruct((4, 4, 2, 8, DIM), BF),) + (jax.ShapeDtypeStruct((ROWS, CACHE, SEQ), BF),) * 2,
        in_specs=[vm] + [pl.BlockSpec(memory_space=pltpu.HBM)] * 11,
        out_specs=(anyspec, vm, vm),
        scratch_shapes=[
            pltpu.VMEM((CACHE, DIM), BF), pltpu.VMEM((DIM, QR), BF), pltpu.VMEM((QR, HEADS * QKD), BF),
            pltpu.VMEM((HEADS, NOPE, KVR), BF), pltpu.VMEM((HEADS, KVR, VD), BF), pltpu.VMEM((HEADS * VD, HALF), BF),
            pltpu.VMEM((DIM, FS), BF), pltpu.VMEM((DIM, FS), BF), pltpu.VMEM((FS, DIM), BF),
            pltpu.VMEM((PAD, DIM), F32), pltpu.VMEM((PAD, KVR + 128), F32),
            pltpu.VMEM((PAD, HEADS * QKD), F32), pltpu.VMEM((ROWS, HP, KVR), F32), pltpu.VMEM((ROWS, HP, 128), F32),
            pltpu.VMEM((PAD, HEADS * VD), F32), pltpu.VMEM((WOC, PAD, KC), BF), pltpu.VMEM((PAD, HALF), F32), pltpu.VMEM((2, PAD, CACHE), BF),
            pltpu.VMEM((2, ROWS, HEADS * VD), BF), pltpu.VMEM((2, ROWS, HEADS * VD), BF), pltpu.VMEM((2, ROWS, DIM), BF), pltpu.VMEM((2, ROWS, DIM), BF),
            pltpu.VMEM((2, 2 * ROWS, HALF), BF), pltpu.VMEM((GROUP, 2 * ROWS, HALF), BF), pltpu.VMEM((GROUP * ROWS, DIM), F32),
            pltpu.VMEM((GROUP * ROWS, DIM), F32), pltpu.VMEM((GROUP, ROWS, DIM), BF), pltpu.VMEM((GROUP, ROWS, DIM), BF),
            pltpu.VMEM((GROUP, GROUP * ROWS, 128), BF), pltpu.VMEM((GROUP, GROUP * ROWS, 128), BF),
            pltpu.VMEM((4, 4, 2, 8, DIM), BF),
            dma((n_loads,)), dma((2, GROUP)), dma((2, GROUP)), dma((2, GROUP)), dma((2, GROUP)),
            dma((2, 2)), dma((2, 2)), dma((64,)), dma((64,)), dma((8,)), dma((8,)), dma((16,)),
        ],
        compiler_params=pltpu.CompilerParams(vmem_limit_bytes=48 * 1024 * 1024, collective_id=0, has_side_effects=True),
        name="two_layers",
    )(pk, cache0, cache1, wdkv, wqa, wqb, wuk, wuv, wo, wg, wu, wd)


def solution(mesh):
    row_spec = P(("replica", "dp"), None)
    len_spec = P(("replica", "dp"))
    cache_spec = P(("replica", "dp"), None, None)
    in_specs = (row_spec, len_spec, cache_spec, cache_spec) + (P(),) * 13
    out_specs = (P("replica", None), cache_spec, cache_spec)

    def device_step(x_rows, lengths, cache0, cache1, attn_gain, w_dkv, kv_gain, wq_a, q_gain, wq_b, w_uk, w_uv, w_o, ffn_gain, w_gate, w_up, w_down):
        half = ROPE // 2
        inv_freq = 10000.0 ** (-(np.arange(128) % half) / half)
        freq = jnp.broadcast_to(jnp.asarray(inv_freq[None, :], F32), (2, 128))
        lens = jnp.broadcast_to(lengths.astype(F32)[:, None], (ROWS, SEQ))
        pk, at = 0.0, 0
        pieces = [x_rows.astype(F32), attn_gain, ffn_gain, kv_gain, q_gain, freq, lens]
        width = sum(piece.shape[1] for piece in pieces)
        for piece in pieces:
            pk = pk + jnp.pad(piece, ((0, 0), (at, width - at - piece.shape[1])))
            at += piece.shape[1]
        x, *kept = two_layers(pk, cache0.transpose(0, 2, 1), cache1.transpose(0, 2, 1),
                           w_dkv.transpose(0, 2, 1), wq_a, wq_b, w_uk, w_uv, w_o, w_gate, w_up, w_down)
        return x.reshape(-1, DIM), kept[0].transpose(0, 2, 1), kept[1].transpose(0, 2, 1)

    return jax.shard_map(device_step, mesh=mesh, in_specs=in_specs, out_specs=out_specs, check_vma=False)
```

```python
import functools

import jax
import jax.numpy as jnp
import numpy as np
from jax import lax
from jax.experimental import pallas as pl
from jax.experimental.pallas import tpu as pltpu
from jax.sharding import PartitionSpec as P

BF = jnp.bfloat16
F32 = jnp.float32
MESH = pl.DeviceIdType.MESH
NT = (((1,), (1,)), ((), ()))

SEQ = 1024
DIM = 2048
FFN = 10240
HEADS = 20
KVR = 512
NOPE = 192
ROPE = 64
QKD = NOPE + ROPE
CACHE = KVR + ROPE
QR = 768
VD = 256
ROWS = 2
PAD = 16
HP = 32
GROUP = 16
HALF = DIM // 2
FS = FFN // GROUP
QB = 4
KC = 1024
WOC = HEADS * VD // KC
AHEAD = 12


AT_X, AT_AG, AT_FG, AT_KV = 0, DIM, 2 * DIM, 3 * DIM
AT_QG = AT_KV + KVR
AT_FREQ = AT_QG + QR
AT_LEN = AT_FREQ + 128


def rms(v, gain):
    return v * lax.rsqrt(jnp.mean(v * v, axis=-1, keepdims=True) + 1e-6) * gain


def rope_lanes(t, cos_t, sin_t):
    lane = lax.broadcasted_iota(jnp.int32, t.shape, 1)
    swapped = jnp.where(lane < ROPE // 2, pltpu.roll(t, 128 - ROPE // 2, 1), pltpu.roll(t, ROPE // 2, 1))
    return t * cos_t + swapped * sin_t


def dev(i):
    return (lax.axis_index("replica"), i)


def remote(src, dst, send_sem, recv_sem, peer):
    return pltpu.make_async_remote_copy(src_ref=src, dst_ref=dst, send_sem=send_sem, recv_sem=recv_sem, device_id=dev(peer), device_id_type=MESH)


def step_kernel(pk_ref, cache0_ref, cache1_ref, wdkv_ref, wqa_ref, wqb_ref, wuk_ref, wuv_ref, wo_ref, wg_ref, wu_ref, wd_ref,
                out_ref, keep0, keep1,
                wdkv, wqa, wqb, wuk, wuv, wo, wg, wu, wd, xs, ks, qf, qlat, qrs, of, ob, acc, entry, osend, orecv, xpart, xsend, xm, xg, xf, pf, ps, pr, ps2, pr2,
                sems, s1, r1, s2, r2, p1, q1, fs, fr, ds, dr):
    idx = lax.axis_index("dp")
    core = lax.rem(idx, 2)
    cx = lax.rem(lax.div(idx, 2), 4)
    cy = lax.rem(lax.div(idx, 8), 4)
    cz = lax.div(idx, 32)
    gx, gy, gz = lax.div(cx, 2), lax.div(cy, 2), lax.div(cz, 2)
    bx, by, bz = lax.rem(cx, 2), lax.rem(cy, 2), lax.rem(cz, 2)
    chip = bz * 4 + by * 2 + bx
    me = chip * 2 + core

    def index(z, y, x, c):
        return z * 32 + y * 8 + x * 2 + c

    def flip(m):
        z = lax.rem(bz + m // 8, 2)
        y = lax.rem(by + m // 4 % 2, 2)
        x = lax.rem(bx + m // 2 % 2, 2)
        c = lax.rem(core + m % 2, 2)
        return z * 8 + y * 4 + x * 2 + c, index(gz * 2 + z, gy * 2 + y, gx * 2 + x, c)

    def away(k):
        return index(lax.rem(cz + lax.div(k, 16), 4), lax.rem(cy + lax.rem(lax.div(k, 4), 4), 4), lax.rem(cx + lax.rem(k, 4), 4), core)

    half = HEADS // 2
    qc = HEADS * QKD // QB
    mine = pl.ds(pl.multiple_of(me * FS, FS), FS)
    my_half = pl.ds(pl.multiple_of(core * HALF, HALF), HALF)
    its_half = pl.ds(pl.multiple_of((1 - core) * HALF, HALF), HALF)
    partner = index(cz, cy, cx, 1 - core)

    def loads_of(layer):
        chunks = [(wdkv_ref.at[layer], wdkv), (wqa_ref.at[layer], wqa)]
        chunks += [(wqb_ref.at[layer, :, pl.ds(i * qc, qc)], wqb.at[:, pl.ds(i * qc, qc)]) for i in range(QB)]
        chunks += [(wuk_ref.at[layer, pl.ds(i * half, half)], wuk.at[pl.ds(i * half, half)]) for i in range(2)]
        chunks += [((cache0_ref, cache1_ref)[layer], (keep0, keep1)[layer])]
        chunks += [(wuv_ref.at[layer, pl.ds(i * half, half)], wuv.at[pl.ds(i * half, half)]) for i in range(2)]
        chunks += [(wo_ref.at[layer, pl.ds(i * KC, KC), my_half], wo.at[pl.ds(i * KC, KC)]) for i in range(WOC)]
        chunks += [(wg_ref.at[layer, :, mine], wg), (wu_ref.at[layer, :, mine], wu), (wd_ref.at[layer, mine, :], wd)]
        return [pltpu.make_async_copy(s, d, sems.at[i]) for i, (s, d) in enumerate(chunks)]

    first_uv = 5 + QB
    first_wo = first_uv + 2
    first_mlp = first_wo + WOC
    loads = [loads_of(0), loads_of(1)]
    for cp in loads[0][:AHEAD]:
        cp.start()

    barrier = pltpu.get_barrier_semaphore()

    def greet(k, carry):
        pl.semaphore_signal(barrier, inc=1, device_id=dev(away(k)), device_id_type=MESH)
        return carry

    lax.fori_loop(1, 64, greet, 0)
    for m in range(1, GROUP, 2):
        pl.semaphore_signal(barrier, inc=1, device_id=dev(flip(m)[1]), device_id_type=MESH)


    lane16 = lax.broadcasted_iota(jnp.int32, (PAD, 128), 1)
    row16 = lax.broadcasted_iota(jnp.int32, (PAD, 128), 0)
    at_len = [pk_ref[b:b + 1, AT_LEN:AT_LEN + SEQ].astype(jnp.int32) for b in range(ROWS)]
    angle = jnp.where(row16 == 0, pk_ref[0:1, AT_LEN:AT_LEN + 128], pk_ref[1:2, AT_LEN:AT_LEN + 128]) * pk_ref[0:1, AT_FREQ:AT_FREQ + 128]
    cos_t = jnp.where(lane16 < ROPE, jnp.cos(angle), 0.0)
    sin_t = jnp.sin(angle)
    sin_t = jnp.where(lane16 < ROPE, jnp.where(lane16 < ROPE // 2, -sin_t, sin_t), 0.0)

    xs[...] = jnp.zeros_like(xs)
    xs[0:ROWS, :] = pk_ref[:, AT_X:AT_X + DIM]
    xsend[0] = pk_ref[:, AT_X:AT_X + DIM].astype(BF)
    ks[...] = jnp.zeros_like(ks)
    of[...] = jnp.zeros_like(of)
    for b in range(ROWS):
        qlat[b, 16:HP, :] = jnp.zeros((HP - 16, KVR), F32)
        qrs[b, 16:HP, :] = jnp.zeros((HP - 16, 128), F32)

    def attention(layer):
        cbuf = (keep0, keep1)[layer]

        def ready(i):
            loads[layer][i].wait()
            if layer == 0 and i + AHEAD < len(loads[0]):
                loads[0][i + AHEAD].start()

        h = rms(xs[...], pk_ref[layer:layer + 1, AT_AG:AT_AG + DIM]).astype(BF)
        ready(0)
        k = lax.dot_general(h, wdkv[...], NT, preferred_element_type=F32)
        ready(1)
        qa = jnp.dot(h, wqa[...], preferred_element_type=F32)
        qa = rms(qa, pk_ref[layer:layer + 1, AT_QG:AT_QG + QR]).astype(BF)
        ks[:, 0:CACHE] = k
        ks[:, 0:KVR] = rms(k[:, 0:KVR], pk_ref[layer:layer + 1, AT_KV:AT_KV + KVR]).astype(BF).astype(F32)
        ks[:, KVR:KVR + 128] = rope_lanes(ks[:, KVR:KVR + 128], cos_t, sin_t).astype(BF).astype(F32)
        entry[layer] = ks[:, 0:CACHE].astype(BF)

        heads_q = HEADS // QB
        qparts = []
        for i in range(QB):
            ready(2 + i)
            qi = jnp.dot(qa, wqb[:, i * qc:(i + 1) * qc], preferred_element_type=F32).astype(BF)
            qf[:, i * qc:(i + 1) * qc] = qi.astype(F32)
            qparts.append(qi)
        for j in range(HEADS):
            if j % half == 0:
                ready(2 + QB + j // half)
            jj = j % heads_q
            qn = qparts[j // heads_q][:, jj * QKD:jj * QKD + NOPE]
            ql = jnp.dot(qn, wuk[j], preferred_element_type=F32)
            for b in range(ROWS):
                qlat[b, j:j + 1, :] = ql[b:b + 1, :]
                qrs[b, j:j + 1, :] = qf[b:b + 1, j * QKD + 128:(j + 1) * QKD]

        ready(4 + QB)
        ol = []
        slot = lax.broadcasted_iota(jnp.int32, (HP, SEQ), 1)
        for b in range(ROWS):
            p = at_len[b]
            ql = qlat[b].astype(BF)
            qr = rope_lanes(pltpu.roll(qrs[b], 64, 1), cos_t[b:b + 1, :], sin_t[b:b + 1, :]).astype(BF)
            s = jnp.dot(ql, cbuf[b, 0:KVR, :], preferred_element_type=F32)
            s += jnp.dot(qr[:, 0:ROPE], cbuf[b, KVR:CACHE, :], preferred_element_type=F32)
            own = jnp.sum(ql.astype(F32) * ks[b:b + 1, 0:KVR], axis=-1, keepdims=True)
            own += jnp.sum(qr.astype(F32) * ks[b:b + 1, KVR:KVR + 128], axis=-1, keepdims=True)
            s = jnp.where(slot == p, own, s) * (QKD ** -0.5)
            s = jnp.where(slot <= p, s, -1e30)
            e = jnp.exp(s - jnp.max(s, axis=-1, keepdims=True))
            a = (e / jnp.sum(e, axis=-1, keepdims=True)).astype(BF)
            af = a.astype(F32)
            a_own = jnp.sum(jnp.where(slot == p, af, 0.0), axis=-1, keepdims=True)
            a_old = jnp.where(slot == p, 0.0, af).astype(BF)
            o = lax.dot_general(a_old, cbuf[b, 0:KVR, :], NT, preferred_element_type=F32)
            ol.append((o + a_own * ks[b:b + 1, 0:KVR]).astype(BF))
        olc = jnp.concatenate(ol, axis=0)
        for j in range(HEADS):
            if j % half == 0:
                ready(first_uv + j // half)
            r = jnp.dot(olc, wuv[j], preferred_element_type=F32)
            for b in range(ROWS):
                of[b:b + 1, j * VD:(j + 1) * VD] = r[b * HP + j:b * HP + j + 1, :]
        osend[layer] = of[0:ROWS, :].astype(BF)
        acc[...] = jnp.zeros_like(acc)
        if layer == 0:
            pl.semaphore_wait(barrier, 63 + GROUP // 2)
            cp = remote(xsend.at[0], xpart.at[0], p1.at[0, 1], q1.at[0, 1], partner)
            cp.start()
            sent.append(cp)
        cp = remote(osend.at[layer], orecv.at[layer], p1.at[layer, 0], q1.at[layer, 0], partner)
        cp.start()
        sent.append(cp)
        cp.wait_recv()
        of[ROWS:2 * ROWS, :] = orecv[layer].astype(F32)
        for i in range(WOC):
            ob[i] = of[:, i * KC:(i + 1) * KC].astype(BF)

        def step(i, carry):
            at = pl.ds(pl.multiple_of(i * KC, KC), KC)
            pltpu.make_async_copy(wo_ref.at[layer, at, my_half], wo.at[at], sems.at[first_wo + i]).wait()
            acc[...] += jnp.dot(ob[i], wo[at, :], preferred_element_type=F32)
            return carry

        lax.fori_loop(0, WOC, step, 0)
        remote(xpart.at[layer], xpart.at[layer], p1.at[layer, 1], q1.at[layer, 1], partner).wait_recv()
        xm[layer, 0:ROWS, :] = (xs[0:ROWS, my_half] + acc[0:ROWS, :]).astype(BF)
        xm[layer, ROWS:2 * ROWS, :] = (xpart[layer, :, my_half].astype(F32) + acc[ROWS:2 * ROWS, :]).astype(BF)

    def insert(layer):
        keep = (keep0, keep1)[layer]

        def tile(t, carry):
            at = pl.ds(pl.multiple_of(t * 128, 128), 128)
            lane = lax.broadcasted_iota(jnp.int32, (CACHE, 128), 1) + t * 128
            for b in range(ROWS):
                hot = jnp.where((row16 == b) & (lane16 + t * 128 == at_len[b][:, 0:128]), 1.0, 0.0).astype(BF)
                col = lax.dot_general(entry[layer], hot, (((0,), (0,)), ((), ())), preferred_element_type=F32)
                keep[b, :, at] = jnp.where(lane == at_len[b][:, 0:128], col, keep[b, :, at].astype(F32)).astype(BF)
            return carry

        lax.fori_loop(0, SEQ // 128, tile, 0)

    def group_rows(layer):
        copies = []
        for m in range(GROUP - 1, 0, -1):
            cp = remote(xm.at[layer], xg.at[me], s1.at[layer, m], r1.at[layer, m], flip(m)[1])
            cp.start()
            copies.append(cp)
        return copies

    def mlp_share(layer):
        xg[me] = xm[layer]
        for m in range(1, GROUP):
            r, peer = flip(m)
            remote(xm.at[layer], xg.at[r], s1.at[layer, m], r1.at[layer, m], peer).wait_recv()
        for d in range(GROUP):
            at = pl.ds(d % 2 * HALF, HALF)
            xf[ROWS * d:ROWS * (d + 1), at] = xg[d, 0:ROWS, :].astype(F32)
            d2 = d + 1 - 2 * (d % 2)
            xf[ROWS * d2:ROWS * (d2 + 1), at] = xg[d, ROWS:2 * ROWS, :].astype(F32)
        g = rms(xf[...], pk_ref[layer:layer + 1, AT_FG:AT_FG + DIM]).astype(BF)
        loads[layer][first_mlp].wait()
        gate = jnp.dot(g, wg[...], preferred_element_type=F32)
        loads[layer][first_mlp + 1].wait()
        up = jnp.dot(g, wu[...], preferred_element_type=F32)
        u = (gate * jax.nn.sigmoid(gate) * up).astype(BF)
        loads[layer][first_mlp + 2].wait()
        pf[...] = jnp.dot(u, wd[...], preferred_element_type=F32)

    sent = []
    attention(0)
    sent += group_rows(0)
    for cp in loads[1][:4 + QB]:
        cp.start()
    mlp_share(0)
    for d in range(GROUP):
        ps[d] = pf[ROWS * d:ROWS * (d + 1), :].astype(BF)
    for m in range(GROUP - 1, 0, -1):
        r, peer = flip(m)
        cp = remote(ps.at[r], pr.at[me], s2.at[0, m], r2.at[0, m], peer)
        cp.start()
        sent.append(cp)
    for cp in loads[1][4 + QB:]:
        cp.start()
    pr[me] = ps[me]
    insert(0)
    for m in range(1, GROUP):
        r, peer = flip(m)
        remote(ps.at[r], pr.at[r], s2.at[0, m], r2.at[0, m], peer).wait_recv()
    total = pr[0].astype(F32)
    for d in range(1, GROUP):
        total += pr[d].astype(F32)
    xs[0:ROWS, my_half] = xg[me, 0:ROWS, :].astype(F32)
    xs[0:ROWS, its_half] = xg[me + 1 - 2 * core, ROWS:2 * ROWS, :].astype(F32)
    new_x = (xs[0:ROWS, :] + total).astype(BF)
    xsend[1] = new_x
    xs[0:ROWS, :] = new_x.astype(F32)
    cp = remote(xsend.at[1], xpart.at[1], p1.at[1, 1], q1.at[1, 1], partner)
    cp.start()
    sent.append(cp)

    attention(1)
    sent += group_rows(1)
    mlp_share(1)
    def cols(q, c):
        return pl.ds(pl.multiple_of(c * 1024 + q * 128, 128), 128)

    for d in range(GROUP):
        ps2[d] = pf[:, (d % 2) * 1024 + d // 2 * 128:(d % 2) * 1024 + d // 2 * 128 + 128].astype(BF)
    for m in range(GROUP - 1, 0, -1):
        r, peer = flip(m)
        cp = remote(ps2.at[r], pr2.at[me], s2.at[1, m], r2.at[1, m], peer)
        cp.start()
        sent.append(cp)
    pr2[me] = ps2[me]
    for m in range(1, GROUP):
        r, peer = flip(m)
        remote(ps2.at[r], pr2.at[r], s2.at[1, m], r2.at[1, m], peer).wait_recv()
    total = pr2[0].astype(F32)
    for d in range(1, GROUP):
        total += pr2[d].astype(F32)
    fin = (xf[:, cols(chip, core)] + total).astype(BF)
    for z in range(2):
        for y in range(2):
            out_ref[gz * 2 + z, gy * 2 + y, gx, :, cols(chip, core)] = fin[(z * 2 + y) * 8:(z * 2 + y) * 8 + 8, :]

    def block(ref, z, y, x, c):
        q = lax.rem(z, 2) * 4 + lax.rem(y, 2) * 2 + lax.rem(x, 2)
        return ref.at[pl.ds(lax.div(z, 2) * 2, 2), pl.ds(lax.div(y, 2) * 2, 2), lax.div(x, 2), :, cols(q, c)]

    def side(ref, z, y, x, c):
        return ref.at[pl.ds(z * 2, 2), pl.ds(y * 2, 2), x, :, pl.ds(pl.multiple_of(c * 1024, 1024), 1024)]

    own_block = block(out_ref, cz, cy, cx, core)

    def digit(a):
        return lax.rem(2 + 3 * a, 4)

    def spread(i, carry):
        k = digit(lax.div(i, 16)) * 16 + digit(lax.rem(lax.div(i, 4), 4)) * 4 + digit(lax.rem(i, 4))

        @pl.when(k != 0)
        def _():
            remote(own_block, own_block, fs.at[k], fr.at[k], away(k)).start()
        return carry

    lax.fori_loop(0, 64, spread, 0)
    insert(1)

    def gathered(t, carry):
        z = lax.rem(gz + lax.div(t, 4), 2)
        y = lax.rem(gy + lax.rem(lax.div(t, 2), 2), 2)
        x = lax.rem(gx + lax.rem(t, 2), 2)

        def arrive(q, carry):
            oz, oy, ox = z * 2 + lax.div(q, 4), y * 2 + lax.rem(lax.div(q, 2), 2), x * 2 + lax.rem(q, 2)
            k = lax.rem(cz + 4 - oz, 4) * 16 + lax.rem(cy + 4 - oy, 4) * 4 + lax.rem(cx + 4 - ox, 4)

            @pl.when(k != 0)
            def _():
                remote(own_block, block(out_ref, oz, oy, ox, core), fs.at[k], fr.at[k], index(oz, oy, ox, core)).wait_recv()
            return carry

        lax.fori_loop(0, 8, arrive, 0)
        part = side(out_ref, z, y, x, core)
        remote(part, part, ds.at[t], dr.at[t], partner).start()
        return carry

    lax.fori_loop(0, 8, gathered, 0)

    def passed(t, carry):
        z = lax.rem(gz + lax.div(t, 4), 2)
        y = lax.rem(gy + lax.rem(lax.div(t, 2), 2), 2)
        x = lax.rem(gx + lax.rem(t, 2), 2)
        part = side(out_ref, z, y, x, 1 - core)
        remote(part, part, ds.at[t], dr.at[t], partner).wait_recv()
        return carry

    lax.fori_loop(0, 8, passed, 0)
    for cp in sent:
        cp.wait_send()

    def sent_block(k, carry):
        remote(own_block, own_block, fs.at[k], fr.at[k], away(k)).wait_send()
        return carry

    lax.fori_loop(1, 64, sent_block, 0)

    def finish(t, carry):
        part = side(out_ref, 0, 0, 0, core)
        remote(part, part, ds.at[t], dr.at[t], partner).wait_send()
        return carry

    lax.fori_loop(0, 8, finish, 0)


def two_layers(pk, cache0, cache1, wdkv, wqa, wqb, wuk, wuv, wo, wg, wu, wd):
    vm = pl.BlockSpec(memory_space=pltpu.VMEM)
    dma = pltpu.SemaphoreType.DMA
    n_loads = 5 + QB + 2 + WOC + 3
    return pl.pallas_call(
        step_kernel,
        out_shape=(jax.ShapeDtypeStruct((4, 4, 2, 8, DIM), BF),) + (jax.ShapeDtypeStruct((ROWS, CACHE, SEQ), BF),) * 2,
        in_specs=[vm] + [pl.BlockSpec(memory_space=pltpu.HBM)] * 11,
        out_specs=(vm, vm, vm),
        scratch_shapes=[
            pltpu.VMEM((CACHE, DIM), BF), pltpu.VMEM((DIM, QR), BF), pltpu.VMEM((QR, HEADS * QKD), BF),
            pltpu.VMEM((HEADS, NOPE, KVR), BF), pltpu.VMEM((HEADS, KVR, VD), BF), pltpu.VMEM((HEADS * VD, HALF), BF),
            pltpu.VMEM((DIM, FS), BF), pltpu.VMEM((DIM, FS), BF), pltpu.VMEM((FS, DIM), BF),
            pltpu.VMEM((PAD, DIM), F32), pltpu.VMEM((PAD, KVR + 128), F32),
            pltpu.VMEM((PAD, HEADS * QKD), F32), pltpu.VMEM((ROWS, HP, KVR), F32), pltpu.VMEM((ROWS, HP, 128), F32),
            pltpu.VMEM((PAD, HEADS * VD), F32), pltpu.VMEM((WOC, PAD, KC), BF), pltpu.VMEM((PAD, HALF), F32), pltpu.VMEM((2, PAD, CACHE), BF),
            pltpu.VMEM((2, ROWS, HEADS * VD), BF), pltpu.VMEM((2, ROWS, HEADS * VD), BF), pltpu.VMEM((2, ROWS, DIM), BF), pltpu.VMEM((2, ROWS, DIM), BF),
            pltpu.VMEM((2, 2 * ROWS, HALF), BF), pltpu.VMEM((GROUP, 2 * ROWS, HALF), BF), pltpu.VMEM((GROUP * ROWS, DIM), F32),
            pltpu.VMEM((GROUP * ROWS, DIM), F32), pltpu.VMEM((GROUP, ROWS, DIM), BF), pltpu.VMEM((GROUP, ROWS, DIM), BF),
            pltpu.VMEM((GROUP, GROUP * ROWS, 128), BF), pltpu.VMEM((GROUP, GROUP * ROWS, 128), BF),
            dma((n_loads,)), dma((2, GROUP)), dma((2, GROUP)), dma((2, GROUP)), dma((2, GROUP)),
            dma((2, 2)), dma((2, 2)), dma((64,)), dma((64,)), dma((8,)), dma((8,)),
        ],
        compiler_params=pltpu.CompilerParams(vmem_limit_bytes=48 * 1024 * 1024, collective_id=0, has_side_effects=True),
        name="two_layers",
    )(pk, cache0, cache1, wdkv, wqa, wqb, wuk, wuv, wo, wg, wu, wd)


def write_kernel(x_ref, c0_ref, c1_ref, xo_ref, o0_ref, o1_ref, sems):
    pairs = [(x_ref, xo_ref)] + [(c.at[b], o.at[b]) for c, o in ((c0_ref, o0_ref), (c1_ref, o1_ref)) for b in range(ROWS)]
    copies = [pltpu.make_async_copy(s, d, sems.at[i]) for i, (s, d) in enumerate(pairs)]
    for cp in copies:
        cp.start()
    for cp in copies:
        cp.wait()


def write_out(x, c0, c1):
    return pl.pallas_call(
        write_kernel,
        out_shape=tuple(jax.ShapeDtypeStruct(v.shape, v.dtype) for v in (x, c0, c1)),
        in_specs=[pl.BlockSpec(memory_space=pltpu.VMEM)] * 3,
        out_specs=(pl.BlockSpec(memory_space=pltpu.HBM),) * 3,
        scratch_shapes=[pltpu.SemaphoreType.DMA((1 + 2 * ROWS,))],
        compiler_params=pltpu.CompilerParams(vmem_limit_bytes=16 * 1024 * 1024),
        name="write_out",
    )(x, c0, c1)


def solution(mesh):
    row_spec = P(("replica", "dp"), None)
    len_spec = P(("replica", "dp"))
    cache_spec = P(("replica", "dp"), None, None)
    in_specs = (row_spec, len_spec, cache_spec, cache_spec) + (P(),) * 13
    out_specs = (P("replica", None), cache_spec, cache_spec)

    def device_step(x_rows, lengths, cache0, cache1, attn_gain, w_dkv, kv_gain, wq_a, q_gain, wq_b, w_uk, w_uv, w_o, ffn_gain, w_gate, w_up, w_down):
        half = ROPE // 2
        inv_freq = 10000.0 ** (-(np.arange(128) % half) / half)
        freq = jnp.broadcast_to(jnp.asarray(inv_freq[None, :], F32), (2, 128))
        lens = jnp.broadcast_to(lengths.astype(F32)[:, None], (ROWS, SEQ))
        pk, at = 0.0, 0
        pieces = [x_rows.astype(F32), attn_gain, ffn_gain, kv_gain, q_gain, freq, lens]
        width = sum(piece.shape[1] for piece in pieces)
        for piece in pieces:
            pk = pk + jnp.pad(piece, ((0, 0), (at, width - at - piece.shape[1])))
            at += piece.shape[1]
        x, *kept = two_layers(pk, cache0.transpose(0, 2, 1), cache1.transpose(0, 2, 1),
                           w_dkv.transpose(0, 2, 1), wq_a, wq_b, w_uk, w_uv, w_o, w_gate, w_up, w_down)
        x, *kept = write_out(x, *kept)
        return x.reshape(-1, DIM), kept[0].transpose(0, 2, 1), kept[1].transpose(0, 2, 1)

    return jax.shard_map(device_step, mesh=mesh, in_specs=in_specs, out_specs=out_specs, check_vma=False)
```
